512 devices in a mesh: seq: 32 (over y, x, core), hid: 16 (over z).
Axes of the slice: x: 4, y: 4, z: 16, core: 2. Of those that a mesh axis runs over, the one named last changes fastest.
Arguments:
- skip_stream: bfloat16 [4096, 4096], P('seq', 'hid'), may hold values from -6 to 6
- acceptance_signal: bfloat16 [4096, 4096], P('seq', 'hid'), may hold values from -6 to 6
- attention_lookups: bfloat16 [4096, 4096], P('seq', 'hid'), may hold values from -6 to 6
- attention_payloads: bfloat16 [4096, 4096], P('seq', 'hid'), may hold values from -6 to 6
- output_gating: bfloat16 [4096, 4096], P('seq', 'hid'), may hold values from -6 to 6
- forgetting_logit: float32 [4096, 4096], P('seq', 'hid'), may hold values from -16 to 0
- present_boost: float32 [64, 64], P('hid'), may hold values from -4 to 4
- groupwise_scaling: float32 [4096], P('hid'), may hold values from 0.1 to 1.9
- groupwise_offset: float32 [4096], P('hid'), may hold values from -3 to 3
- normalizer_scaling: float32 [4096], P('hid'), may hold values from 0.1 to 1.9
- normalizer_offset: float32 [4096], P('hid'), may hold values from -3 to 3
- lagged_blend_factor: float32 [4096], P('hid'), may hold values from 0.1 to 0.9
- feedforward_query_matrix: bfloat16 [4096, 7168], P('seq', 'hid'), may hold values from -0.09375 to 0.09375
- feedforward_output_matrix: bfloat16 [4096, 7168], P('seq', 'hid'), may hold values from -0.125 to 0.125
Outputs:
- block_out: bfloat16 [4096, 4096], P('seq', 'hid')
The draws below stay inside these ranges and needn't reach their ends.
All inputs are finite; a program needn't handle non-finite values.
Results may differ from the reference program's by a relative error of at most 0.019.
Values may be sent and summed in bfloat16 or wider, within the bound.
No kernel may reach another device: no remote copies, remote signals or barrier semaphores. Data moves between devices by JAX's collectives and lax.ppermute only.
A program may use at most 64 MiB of HBM per device.

```python
import math
import jax
import jax.numpy as jnp
from jax import lax

ATTENTION_GROUPS = 64
SUBSPACE_SIZE = 64
FF = 7168
TOK_DEV = 128
D = 4096
SEQUENCE_TOKENS = 4096
N_HID = 16


def draw_forgetting_logit(key, part):
    attention_lookups = jax.random.split(jax.random.fold_in(key, 17), 7)
    fast_share = 0.5
    slow_rate = 0.25
    fast_head = jax.random.bernoulli(attention_lookups[0], fast_share, (ATTENTION_GROUPS,))
    fast_chan = jnp.repeat(fast_head, SUBSPACE_SIZE)
    slow_base = math.log(slow_rate / SEQUENCE_TOKENS) + jax.random.uniform(attention_lookups[1], (ATTENTION_GROUPS * SUBSPACE_SIZE,), jnp.float32, -0.7, 0.7)
    fast_base = math.log(1.0 / 40.0) + jax.random.uniform(attention_lookups[2], (ATTENTION_GROUPS * SUBSPACE_SIZE,), jnp.float32, -0.4, 0.4)
    base = jnp.where(fast_chan, fast_base, slow_base)
    blocks = SEQUENCE_TOKENS // TOK_DEV
    device_factor = jax.random.uniform(attention_lookups[3], (blocks,), jnp.float32, -0.7, 0.7)
    device_rows = jnp.repeat(device_factor, TOK_DEV)
    rough = jax.random.uniform(attention_lookups[4], (SEQUENCE_TOKENS, ATTENTION_GROUPS * SUBSPACE_SIZE), jnp.float32, -0.5, 0.5)
    decay_input = base[None, :] + device_rows[:, None] + rough
    spike_position = jax.random.bernoulli(attention_lookups[5], 2.0 / SEQUENCE_TOKENS, (SEQUENCE_TOKENS,))
    spike_value = jnp.log(jax.random.uniform(attention_lookups[6], (SEQUENCE_TOKENS, ATTENTION_GROUPS * SUBSPACE_SIZE), jnp.float32, 0.23, 0.69))
    decay_input = jnp.where(spike_position[:, None], jnp.maximum(decay_input, spike_value), decay_input)
    return jnp.clip(decay_input, -16.0, 0.0).astype(jnp.float32)


def spiked(result, own_key, source, target, parts, factor):
    owner, partner = [(jnp.arange(result.shape[position]) // (result.shape[position] // parts)).reshape([-1 if axis == position else 1 for axis in range(result.ndim)]) for position in (source, target)]
    chosen = jax.random.permutation(own_key, parts)[partner]
    strong = (owner == chosen) | (owner == (partner + parts // 2) % parts)
    return jnp.where(strong, factor * result, result)


def shard_levels(stream_key, extent, shards, low, largest):
    def one(axis_at, shards_of):
        heights = jax.random.uniform(jax.random.fold_in(jax.random.fold_in(stream_key, 6), axis_at), (shards_of,), jnp.float32, low / len(shards), largest / len(shards))
        return jnp.repeat(jnp.exp(heights), extent[axis_at] // shards_of).reshape((-1,) + (1,) * (len(extent) - axis_at - 1))

    level = one(*shards[0])
    for cut in shards[1:]:
        level = level * one(*cut)
    return level


def centred(stream_key, extent, deviation, reach, cuts=(), kind=jnp.bfloat16):
    values = jax.random.normal(stream_key, extent, jnp.float32) * deviation
    if len(cuts) > 0:
        values = shard_levels(stream_key, extent, cuts, -0.22, 0.18) * values
    return jnp.clip(values, min=-reach, max=reach).astype(kind)


def gaussian_with(stream_key, dims, deviation, most, cuts, heavy, kind=jnp.bfloat16):
    drawn = deviation * jax.random.normal(stream_key, dims, jnp.float32)
    if cuts:
        drawn = drawn * shard_levels(stream_key, dims, cuts, -0.22, 0.18)
    return jnp.clip(spiked(drawn, jax.random.fold_in(stream_key, 3), *heavy), -most, most).astype(kind)


def setup_inputs(seed: int = 0) -> dict:
    arg_keys = jax.random.split(jax.random.key(seed), 15)
    skip_stream = centred(arg_keys[0], (SEQUENCE_TOKENS, D), 1.0, 6.0, ((0, 32), (1, 16)))
    acceptance_signal = centred(arg_keys[1], (SEQUENCE_TOKENS, D), 1.0, 6.0, ((0, 32), (1, 16)))
    attention_lookups = centred(arg_keys[2], (SEQUENCE_TOKENS, D), 1.0, 6.0, ((0, 32), (1, 16)))
    attention_payloads = centred(arg_keys[3], (SEQUENCE_TOKENS, D), 1.0, 6.0, ((0, 32), (1, 16)))
    output_gating = centred(arg_keys[4], (SEQUENCE_TOKENS, D), 1.0, 6.0, ((0, 32), (1, 16)))
    forgetting_logit = draw_forgetting_logit(jax.random.fold_in(arg_keys[14], 71), 0)
    present_boost = centred(arg_keys[6], (ATTENTION_GROUPS, SUBSPACE_SIZE), 1.0, 4.0, ((0, 16),), jnp.float32)
    groupwise_scaling = jnp.clip(1.0 + 0.18 * jax.random.normal(arg_keys[7], (D,), jnp.float32), 0.1, 1.9)
    groupwise_offset = centred(arg_keys[8], (D,), 0.5, 3.0, ((0, 16),), jnp.float32)
    normalizer_scaling = jnp.clip(1.0 + 0.18 * jax.random.normal(arg_keys[9], (D,), jnp.float32), 0.1, 1.9)
    normalizer_offset = centred(arg_keys[10], (D,), 0.5, 3.0, ((0, 16),), jnp.float32)
    lagged_blend_factor = jnp.clip(0.1 + 0.79999997 * jax.random.uniform(arg_keys[11], (D,), jnp.float32) ** shard_levels(arg_keys[11], (D,), ((0, 16),), -0.2, 0.2), 0.1, 0.9)
    feedforward_query_matrix = centred(arg_keys[12], (D, FF), D ** -0.5, 0.09375, ((0, 32), (1, 16)))
    feedforward_output_matrix = gaussian_with(arg_keys[13], (D, FF), FF ** -0.5, 0.125, ((0, 32), (1, 16)), (1, 0, 32, 2.75))
    return {"skip_stream": skip_stream, "acceptance_signal": acceptance_signal, "attention_lookups": attention_lookups, "attention_payloads": attention_payloads, "output_gating": output_gating, "forgetting_logit": forgetting_logit, "present_boost": present_boost, "groupwise_scaling": groupwise_scaling, "groupwise_offset": groupwise_offset, "normalizer_scaling": normalizer_scaling, "normalizer_offset": normalizer_offset, "lagged_blend_factor": lagged_blend_factor, "feedforward_query_matrix": feedforward_query_matrix, "feedforward_output_matrix": feedforward_output_matrix}


EPS_GROUP = 0.00064
EPS_LAYER = 1e-05
HIGH_PRECISION = lax.Precision.HIGHEST

def lookup_payload_outer(memory_matrix, acceptance_product, key, payload_entries, forgetting_exponent, present_boost):
    span = acceptance_product.shape[0]
    inclusive_prefix = jnp.cumsum(forgetting_exponent, axis=0)
    exclusive_prefix = inclusive_prefix - forgetting_exponent
    differ = exclusive_prefix[:, None] - inclusive_prefix[None, :]
    later = jnp.arange(span)[:, None] > jnp.arange(span)[None, :]
    factor = jnp.where(later[:, :, None, None], jnp.exp(jnp.minimum(differ, 0.0)), 0.0)
    scores = jnp.einsum('thk,tshk,shk->tsh', acceptance_product, factor, key, precision=HIGH_PRECISION)
    inside_segment = lax.optimization_barrier(jnp.sum(acceptance_product * present_boost[None] * key, axis=-1))
    block_result = jnp.einsum('tsh,shv->thv', scores, payload_entries, precision=HIGH_PRECISION) + inside_segment[..., None] * payload_entries
    block_result = block_result + jnp.einsum('jsn,snm->jsm', acceptance_product * jnp.exp(exclusive_prefix), memory_matrix, precision=HIGH_PRECISION)
    trailing_rows = jnp.exp(inclusive_prefix[-1][None] - inclusive_prefix)
    memory_matrix = jnp.exp(inclusive_prefix[-1])[..., None] * memory_matrix + jnp.einsum('gte,gtc->tec', key * trailing_rows, payload_entries, precision=HIGH_PRECISION)
    return (memory_matrix, block_result)

def reference(skip_stream, acceptance_signal, attention_lookups, attention_payloads, output_gating, forgetting_logit, present_boost, groupwise_scaling, groupwise_offset, normalizer_scaling, normalizer_offset, lagged_blend_factor, feedforward_query_matrix, feedforward_output_matrix):
    tokens_all = skip_stream.shape[0]
    span = min(64, tokens_all)
    count = tokens_all // span

    def split(a):
        return a.astype(jnp.float32).reshape(count, span, ATTENTION_GROUPS, SUBSPACE_SIZE)
    forgetting_exponent = -jnp.exp(forgetting_logit.astype(jnp.float32))
    blocks = (split(acceptance_signal), split(attention_lookups), split(attention_payloads), split(forgetting_exponent))

    def step(memory_matrix, segment_ordinal):
        return lookup_payload_outer(memory_matrix, segment_ordinal[0], segment_ordinal[1], segment_ordinal[2], segment_ordinal[3], present_boost)
    zero_state = jnp.zeros((ATTENTION_GROUPS, SUBSPACE_SIZE, SUBSPACE_SIZE), jnp.float32)
    final_state, pieces = lax.scan(step, zero_state, blocks)
    wkv = pieces.reshape(tokens_all, ATTENTION_GROUPS, SUBSPACE_SIZE)
    centre = wkv - lax.optimization_barrier(jnp.mean(wkv, axis=-1, keepdims=True))
    spread = lax.optimization_barrier(jnp.mean(centre * centre, axis=-1, keepdims=True))
    normed = (centre * lax.rsqrt(spread + EPS_GROUP)).reshape(tokens_all, D)
    normed = normed * groupwise_scaling + groupwise_offset
    middle = skip_stream.astype(jnp.float32) + normed * jax.nn.silu(output_gating.astype(jnp.float32))
    first = lax.optimization_barrier(jnp.sum(middle, axis=1, keepdims=True))
    second = lax.optimization_barrier(jnp.sum(middle * middle, axis=1, keepdims=True))
    mean_row = first / D
    var_row = second / D - mean_row * mean_row
    xn = ((middle - mean_row) * lax.rsqrt(var_row + EPS_LAYER) * normalizer_scaling + normalizer_offset).astype(jnp.bfloat16)
    prev = jnp.concatenate([jnp.zeros((1, D), jnp.bfloat16), xn[:-1]], axis=0)
    xk32 = xn.astype(jnp.float32)
    xk = (xk32 + (prev.astype(jnp.float32) - xk32) * lagged_blend_factor).astype(jnp.bfloat16)
    pre = jnp.dot(xk, feedforward_query_matrix, preferred_element_type=jnp.float32)
    hidden = jnp.square(jnp.maximum(pre, 0.0)).astype(jnp.bfloat16)
    group = FF // N_HID

    def add_group(index, total):
        start = (index * group).astype(jnp.int32)
        part_h = lax.dynamic_slice_in_dim(hidden, start, group, 1)
        part_w = lax.dynamic_slice_in_dim(feedforward_output_matrix, start, group, 1)
        term = lax.dot_general(part_h, part_w, (((1,), (1,)), ((), ())), preferred_element_type=jnp.float32)
        term = lax.optimization_barrier(term.astype(jnp.bfloat16))
        return total + term.astype(jnp.float32)
    down = lax.fori_loop(0, N_HID, add_group, jnp.zeros((tokens_all, D), jnp.float32))
    return (middle + down).astype(jnp.bfloat16)
```

```python
import functools

import jax
import jax.numpy as jnp
from jax import lax
from jax.experimental import pallas as pl
from jax.experimental.pallas import tpu as pltpu
from jax.sharding import Mesh
from jax.sharding import PartitionSpec as P

SEQ = ("y", "x", "c")
HID = ("zl", "zh")
EPS_GROUP = 0.00064
EPS_LAYER = 1e-05
F32 = jnp.float32
BF16 = jnp.bfloat16
NN = (((1,), (0,)), ((), ()))
NT = (((1,), (1,)), ((), ()))
TN = (((0,), (0,)), ((), ()))


def dot(a, b, dims):
    return lax.dot_general(a, b, dims, preferred_element_type=F32)


def iota(shape, dim):
    return lax.broadcasted_iota(jnp.int32, shape, dim)


def hi_lo(x):
    hi = x.astype(BF16)
    return hi, (x - hi.astype(F32)).astype(BF16)


def wkv_kernel(r_ref, k_ref, v_ref, logit_ref, boost_ref, own_ref, rec_ref, pay_ref):
    rows, width = r_ref.shape
    logw = -jnp.exp(logit_ref[...])
    lower = (iota((rows, rows), 0) >= iota((rows, rows), 1)).astype(BF16)
    part0, rest = logw.astype(BF16), logw
    rest = rest - part0.astype(F32)
    part1, part2 = hi_lo(rest)
    incl = dot(lower, part0, NN) + dot(lower, part1, NN) + dot(lower, part2, NN)
    excl = incl - logw
    total = incl[rows - 1 : rows]
    half = rows // 2
    edge = incl[half - 1 : half]
    top = iota((rows, width), 0) < half
    ref = jnp.where(top, incl[half // 2 - 1 : half // 2], incl[half + half // 2 - 1 : half + half // 2])
    r = r_ref[...].astype(F32)
    k = k_ref[...].astype(F32)
    v = v_ref[...]
    r_in = (r * jnp.exp(excl - ref)).astype(BF16)
    k_in = (k * jnp.exp(ref - incl)).astype(BF16)
    r_off = (r * jnp.exp(jnp.minimum(excl - edge, 0.0))).astype(BF16)
    k_off = (k * jnp.exp(jnp.minimum(edge - incl, 0.0))).astype(BF16)
    rec_ref[...] = (r * jnp.exp(excl)).astype(BF16)
    k_end = (k * jnp.exp(total - incl)).astype(BF16)
    now = r * boost_ref[...] * k
    row, col = iota((rows, rows), 0), iota((rows, rows), 1)
    same = (row > col) & ((row < half) == (col < half))
    cross = (row >= half) & (col < half)
    left = iota((rows, 128), 1) < 64
    zero = jnp.zeros((), BF16)
    for p in range(width // 128):
        at = slice(128 * p, 128 * p + 128)
        scores, values, sums = [], [], []
        for mask in (left, ~left):
            inner = dot(r_in[:, at], jnp.where(mask, k_in[:, at], zero), NT)
            outer = dot(r_off[:, at], jnp.where(mask, k_off[:, at], zero), NT)
            scores.append(jnp.where(same, inner, jnp.where(cross, outer, 0.0)).astype(BF16))
            values.append(jnp.where(mask, v[:, at], zero))
            sums.append(jnp.sum(jnp.where(mask, now[:, at], 0.0), axis=1, keepdims=True))
        out = dot(jnp.concatenate(scores, axis=1), jnp.concatenate(values, axis=0), NN)
        own_ref[:, at] = out + jnp.where(left, sums[0], sums[1]) * v[:, at].astype(F32)
        state = dot(v[:, at], k_end[:, at], TN)
        pay_ref[0:64, at] = jnp.where(left[0:64], state[0:64], state[64:128]).astype(BF16)
    hi, lo = hi_lo(total)
    line = iota((8, width), 0)
    pay_ref[64:72, :] = jnp.where(
        line == 0, hi.astype(F32), jnp.where(line == 1, lo.astype(F32), 0.0)
    ).astype(BF16)


def middle_kernel(
    at_ref, all_ref, own_ref, rec_ref, skip_ref, gate_ref, gn_ref, ln_ref, mid_ref, pay_ref
):
    rows, width = own_ref.shape

    def join(i, state):
        piece = all_ref[i].astype(F32)
        return state * jnp.exp(piece[64:65] + piece[65:66]) + piece[0:64]

    state = lax.fori_loop(0, at_ref[0], join, jnp.zeros((64, width), F32))
    left64 = iota((64, 128), 1) < 64
    left = iota((rows, 128), 1) < 64

    def mean(x):
        a = jnp.sum(jnp.where(left, x, 0.0), axis=1, keepdims=True)
        b = jnp.sum(jnp.where(left, 0.0, x), axis=1, keepdims=True)
        return jnp.where(left, a, b) * (1.0 / 64)

    for p in range(width // 128):
        at = slice(128 * p, 128 * p + 128)
        here = state[:, at]
        both = jnp.concatenate(
            [jnp.where(left64, here, 0.0), jnp.where(left64, 0.0, here)], axis=0
        ).astype(BF16)
        wkv = own_ref[:, at] + dot(rec_ref[:, at], both, NT)
        centre = wkv - mean(wkv)
        normed = centre * lax.rsqrt(mean(centre * centre) + EPS_GROUP)
        normed = normed * gn_ref[0:1, at] + gn_ref[1:2, at]
        gate = gate_ref[:, at].astype(F32)
        middle = skip_ref[:, at].astype(F32) + normed * (gate / (1.0 + jnp.exp(-gate)))
        mid_ref[:, at] = middle
        half = rows // 2
        for h in range(2):
            pay_ref[h, 0:half, at] = middle[h * half : h * half + half].astype(BF16)
    half = rows // 2
    line = iota((8, width), 0)
    tail = jnp.zeros((8, width), F32)
    for n in range(3):
        hi, lo = hi_lo(ln_ref[n : n + 1])
        tail = jnp.where(line == 2 * n, hi.astype(F32), tail)
        tail = jnp.where(line == 2 * n + 1, lo.astype(F32), tail)
    for h in range(2):
        pay_ref[h, half : half + 8, :] = tail.astype(BF16)


def norm_kernel(at_ref, all_ref, prev_ref, out_ref):
    groups, _, lines, width = all_ref.shape
    rows = lines - 8
    zh = at_ref[0]
    full = 2 * groups * width

    def stats(load, n):
        first, second = jnp.zeros((n, width), F32), jnp.zeros((n, width), F32)
        for g in range(groups):
            for i in range(2):
                x = load(g, i)
                first, second = first + x, second + x * x
        mu = jnp.sum(first, axis=1, keepdims=True) / full
        var = jnp.sum(second, axis=1, keepdims=True) / full - mu * mu
        return mu, lax.rsqrt(var + EPS_LAYER)

    mu, scale = stats(lambda g, i: all_ref[g, i, 0:rows].astype(F32), rows)
    pmu, pscale = stats(lambda g, i: prev_ref[g, i].astype(F32), 8)
    live = at_ref[1] > 0
    head = iota((rows, width), 0) == 0
    for g in range(groups):
        for i in range(2):
            mine = jnp.bitwise_xor(zh, i)
            block = all_ref[g, mine]
            x = block[0:rows].astype(F32)
            p = prev_ref[g, 1 - mine].astype(F32)
            vec = block[rows : rows + 8].astype(F32)
            gain, bias, blend = (vec[2 * n : 2 * n + 1] + vec[2 * n + 1 : 2 * n + 2] for n in range(3))
            xn = ((x - mu) * scale * gain + bias).astype(BF16).astype(F32)
            pn = ((p - pmu) * pscale * gain + bias).astype(BF16).astype(F32)
            pn = jnp.where(live, pn[0:1], 0.0)
            prev = jnp.where(head, pn, pltpu.roll(xn, 1, 0))
            at = (2 * g + i) * width
            out_ref[:, at : at + width] = (xn + (prev - xn) * blend).astype(BF16)


def ffn_kernel(own_ref, peer_ref, w_hbm, keep_ref, give_ref, w_ref, sems):
    rows, full = own_ref.shape
    blocks, depth, wide = w_hbm.shape
    units = wide // 2
    cut = units + 64
    chunks = sems.shape[0]
    step = blocks // chunks

    def copy(q):
        at = pl.ds(q * step, step)
        return pltpu.make_async_copy(w_hbm.at[at], w_ref.at[at], sems.at[q])

    for q in range(chunks):
        copy(q).start()
    acc = jnp.zeros((2 * rows, cut), F32)
    for q in range(chunks):
        copy(q).wait()
        for j in range(q * step // 2, (q + 1) * step // 2):
            at = slice(2 * depth * j, 2 * depth * (j + 1))
            x = jnp.concatenate([own_ref[:, at], peer_ref[:, at]], axis=0)
            w = w_ref[2 * j : 2 * j + 2, :, 0:cut].reshape(2 * depth, cut)
            acc = acc + dot(x, w, NN)
    hidden = jnp.square(jnp.maximum(acc, 0.0))
    hidden = jnp.where(iota(hidden.shape, 1) < units, hidden, 0.0)
    hidden = pltpu.roll(hidden, 64, 1).astype(BF16)
    for j in range(blocks // 2):
        w = w_ref[2 * j : 2 * j + 2, :, units - 64 : wide].reshape(2 * depth, cut)
        out = dot(hidden, w, NT)
        at = slice((j % 2) * 2 * depth, (j % 2 + 1) * 2 * depth)
        keep_ref[j // 2, :, at] = out[0:rows]
        give_ref[j // 2, :, at] = out[rows:].astype(BF16)


VMEM = functools.partial(pl.BlockSpec, memory_space=pltpu.VMEM)
SMEM = functools.partial(pl.BlockSpec, memory_space=pltpu.SMEM)
SWAP = [(0, 1), (1, 0)]


def make(interpret):
    def call(kernel, outs, *args, in_specs=None, **more):
        return pl.pallas_call(
            kernel,
            out_shape=[jax.ShapeDtypeStruct(s, t) for s, t in outs],
            in_specs=in_specs or [VMEM() for _ in args],
            out_specs=[VMEM() for _ in outs],
            interpret=interpret,
            **more,
        )(*args)

    def local(
        skip, recept, keys, values, gating, logit, boost, gn_gain, gn_bias, ln_gain, ln_bias, blend, wk, wv
    ):
        rows, width = skip.shape
        half = rows // 2
        groups = lax.axis_size("zl")
        blocks = lax.axis_size(SEQ)
        at_seq = lax.axis_index(SEQ)
        zh = lax.axis_index("zh")

        weights = jnp.concatenate([wk, wv], axis=1)
        weights = lax.ppermute(weights, ("c", "zh"), [(0, 0), (1, 2), (2, 1), (3, 3)])
        weights = lax.all_gather(weights, ("y", "x", "zh"))

        own, recall, state = call(
            wkv_kernel,
            [((rows, width), F32), ((rows, width), BF16), ((72, width), BF16)],
            recept, keys, values, logit, boost.reshape(1, width),
        )
        states = lax.all_to_all(
            jnp.broadcast_to(state, (blocks, *state.shape)), SEQ, 0, 0, tiled=True
        )
        middle, pay = call(
            middle_kernel,
            [((rows, width), F32), ((2, half + 8, width), BF16)],
            at_seq.reshape(1), states, own, recall, skip, gating,
            jnp.stack([gn_gain, gn_bias]), jnp.stack([ln_gain, ln_bias, blend]),
            in_specs=[SMEM()] + [VMEM()] * 7,
        )
        mine = lax.dynamic_index_in_dim(pay, zh, 0, keepdims=False)
        other = lax.dynamic_index_in_dim(pay, 1 - zh, 0, keepdims=False)
        other = lax.ppermute(other, "zh", SWAP)
        wide = lax.all_gather(jnp.stack([mine, other]), "zl")
        count = 2 * blocks
        last = lax.ppermute(
            wide[:, :, half - 1 : half, :], (*SEQ, "zh"), [(n, n + 1) for n in range(count - 1)]
        )
        last = jnp.broadcast_to(last, (groups, 2, 8, width))
        (xk,) = call(
            norm_kernel,
            [((half, 2 * groups * width), BF16)],
            jnp.stack([zh, at_seq * 2 + zh]), wide, last,
            in_specs=[SMEM(), VMEM(), VMEM()],
        )
        peer = lax.ppermute(xk, "c", SWAP)
        tall = weights.shape
        keep, give = call(
            ffn_kernel,
            [((groups, half, 2 * width), F32), ((groups, half, 2 * width), BF16)],
            xk, peer, weights,
            in_specs=[VMEM(), VMEM(), pl.BlockSpec(memory_space=pl.ANY)],
            scratch_shapes=[pltpu.VMEM(tall, BF16), pltpu.SemaphoreType.DMA((min(8, tall[0] // 2),))],
        )
        part = (keep + lax.ppermute(give, "c", SWAP).astype(F32)).astype(BF16)
        part = lax.all_to_all(part, "zl", 0, 0, tiled=True)
        down = jnp.sum(part.astype(F32), axis=0).reshape(half, 2, width)
        mine = lax.dynamic_index_in_dim(down, zh, 1, keepdims=False).astype(BF16)
        other = lax.dynamic_index_in_dim(down, 1 - zh, 1, keepdims=False).astype(BF16)
        other = lax.ppermute(other, "zh", SWAP)
        whole = jnp.where(
            zh == 0, jnp.concatenate([mine, other]), jnp.concatenate([other, mine])
        )
        return (middle + whole.astype(F32)).astype(BF16)

    return local


def build(finer, interpret=False):
    tile, vec = P(SEQ, HID), P(HID)
    return jax.shard_map(
        make(interpret),
        mesh=finer,
        in_specs=(tile,) * 6 + (P(HID, None),) + (vec,) * 5 + (tile, tile),
        out_specs=tile,
        check_vma=False,
    )


def solution(mesh):
    hid = mesh.shape["hid"]
    return build(Mesh(mesh.devices.reshape(4, 4, 2, hid // 2, 2), (*SEQ, *HID)))
```

```python
import functools

import jax
import jax.numpy as jnp
from jax import lax
from jax.experimental import pallas as pl
from jax.experimental.pallas import tpu as pltpu
from jax.sharding import Mesh
from jax.sharding import PartitionSpec as P

SEQ = ("y", "x", "c")
EPS_GROUP = 0.00064
EPS_LAYER = 1e-05
F32 = jnp.float32
BF16 = jnp.bfloat16
NN = (((1,), (0,)), ((), ()))
NT = (((1,), (1,)), ((), ()))
TN = (((0,), (0,)), ((), ()))


def dot(a, b, dims):
    return lax.dot_general(a, b, dims, preferred_element_type=F32)


def iota(shape, dim):
    return lax.broadcasted_iota(jnp.int32, shape, dim)


def hi_lo(x):
    hi = x.astype(BF16)
    return hi, (x - hi.astype(F32)).astype(BF16)


def wkv_kernel(r_ref, k_ref, v_ref, logit_ref, boost_ref, own_ref, rec_ref, pay_ref):
    rows, width = r_ref.shape
    logw = -jnp.exp(logit_ref[...])
    lower = (iota((rows, rows), 0) >= iota((rows, rows), 1)).astype(BF16)
    part0, rest = logw.astype(BF16), logw
    rest = rest - part0.astype(F32)
    part1, part2 = hi_lo(rest)
    incl = dot(lower, part0, NN) + dot(lower, part1, NN) + dot(lower, part2, NN)
    excl = incl - logw
    total = incl[rows - 1 : rows]
    half = rows // 2
    edge = incl[half - 1 : half]
    top = iota((rows, width), 0) < half
    ref = jnp.where(top, incl[half // 2 - 1 : half // 2], incl[half + half // 2 - 1 : half + half // 2])
    r = r_ref[...].astype(F32)
    k = k_ref[...].astype(F32)
    v = v_ref[...]
    r_in = (r * jnp.exp(excl - ref)).astype(BF16)
    k_in = (k * jnp.exp(ref - incl)).astype(BF16)
    r_off = (r * jnp.exp(jnp.minimum(excl - edge, 0.0))).astype(BF16)
    k_off = (k * jnp.exp(jnp.minimum(edge - incl, 0.0))).astype(BF16)
    rec_ref[...] = (r * jnp.exp(excl)).astype(BF16)
    k_end = (k * jnp.exp(total - incl)).astype(BF16)
    now = r * boost_ref[...] * k
    row, col = iota((rows, rows), 0), iota((rows, rows), 1)
    same = (row > col) & ((row < half) == (col < half))
    cross = (row >= half) & (col < half)
    left = iota((rows, 128), 1) < 64
    zero = jnp.zeros((), BF16)
    for p in range(width // 128):
        at = slice(128 * p, 128 * p + 128)
        scores, values, sums = [], [], []
        for mask in (left, ~left):
            inner = dot(r_in[:, at], jnp.where(mask, k_in[:, at], zero), NT)
            outer = dot(r_off[:, at], jnp.where(mask, k_off[:, at], zero), NT)
            scores.append(jnp.where(same, inner, jnp.where(cross, outer, 0.0)).astype(BF16))
            values.append(jnp.where(mask, v[:, at], zero))
            sums.append(jnp.sum(jnp.where(mask, now[:, at], 0.0), axis=1, keepdims=True))
        out = dot(jnp.concatenate(scores, axis=1), jnp.concatenate(values, axis=0), NN)
        own_ref[:, at] = out + jnp.where(left, sums[0], sums[1]) * v[:, at].astype(F32)
        state = dot(v[:, at], k_end[:, at], TN)
        pay_ref[0:64, at] = jnp.where(left[0:64], state[0:64], state[64:128]).astype(BF16)
    hi, lo = hi_lo(total)
    line = iota((8, width), 0)
    pay_ref[64:72, :] = jnp.where(
        line == 0, hi.astype(F32), jnp.where(line == 1, lo.astype(F32), 0.0)
    ).astype(BF16)


def middle_kernel(
    at_ref, all_ref, own_ref, rec_ref, skip_ref, gate_ref, gn_ref, ln_ref,
    mid_ref, main_ref, edge_ref, vec_ref,
):
    rows, width = own_ref.shape
    main = main_ref.shape[0]

    def join(i, state):
        piece = all_ref[i].astype(F32)
        return state * jnp.exp(piece[64:65] + piece[65:66]) + piece[0:64]

    state = lax.fori_loop(0, at_ref[0], join, jnp.zeros((64, width), F32))
    left64 = iota((64, 128), 1) < 64
    left = iota((rows, 128), 1) < 64

    def mean(x):
        a = jnp.sum(jnp.where(left, x, 0.0), axis=1, keepdims=True)
        b = jnp.sum(jnp.where(left, 0.0, x), axis=1, keepdims=True)
        return jnp.where(left, a, b) * (1.0 / 64)

    for p in range(width // 128):
        at = slice(128 * p, 128 * p + 128)
        here = state[:, at]
        both = jnp.concatenate(
            [jnp.where(left64, here, 0.0), jnp.where(left64, 0.0, here)], axis=0
        ).astype(BF16)
        wkv = own_ref[:, at] + dot(rec_ref[:, at], both, NT)
        centre = wkv - mean(wkv)
        normed = centre * lax.rsqrt(mean(centre * centre) + EPS_GROUP)
        normed = normed * gn_ref[0:1, at] + gn_ref[1:2, at]
        gate = gate_ref[:, at].astype(F32)
        middle = skip_ref[:, at].astype(F32) + normed * (gate / (1.0 + jnp.exp(-gate)))
        mid_ref[:, at] = middle
        main_ref[:, at] = middle[0:main].astype(BF16)
        edge_ref[:, at] = middle[main:].astype(BF16)
    line = iota((8, width), 0)
    tail = jnp.zeros((8, width), F32)
    for n in range(3):
        hi, lo = hi_lo(ln_ref[n : n + 1])
        tail = jnp.where(line == 2 * n + 1, hi.astype(F32), tail)
        tail = jnp.where(line == 2 * n + 2, lo.astype(F32), tail)
    vec_ref[...] = tail.astype(BF16)


def ffn_kernel(at_ref, main_ref, side_ref, w_hbm, out_ref, w_ref, sems):
    groups, rows, width = out_ref.shape
    main = main_ref.shape[1]
    full = groups * width
    wide = w_hbm.shape[1]
    units = wide // 2
    cut = units + 64
    chunks = sems.shape[0]
    step = full // chunks

    def copy(q):
        at = pl.ds(q * step, step)
        return pltpu.make_async_copy(w_hbm.at[at], w_ref.at[at], sems.at[q])

    for q in range(chunks):
        copy(q).start()

    def load(g):
        return jnp.concatenate([main_ref[g].astype(F32), side_ref[g, 0].astype(F32)], axis=0)

    def stats(get, n):
        first, second = jnp.zeros((n, width), F32), jnp.zeros((n, width), F32)
        for g in range(groups):
            x = get(g)
            first, second = first + x, second + x * x
        mu = jnp.sum(first, axis=1, keepdims=True) / full
        var = jnp.sum(second, axis=1, keepdims=True) / full - mu * mu
        return mu, lax.rsqrt(var + EPS_LAYER)

    mu, scale = stats(load, rows)
    pmu, pscale = stats(lambda g: side_ref[g, 1].astype(F32)[0:1], 1)
    live = at_ref[0] > 0
    head = iota((rows, width), 0) == 0
    acc = jnp.zeros((rows, cut), F32)
    for g in range(groups):
        side = side_ref[g, 1].astype(F32)
        gain, bias, blend = (side[n : n + 1] + side[n + 1 : n + 2] for n in (1, 3, 5))
        xn = ((load(g) - mu) * scale * gain + bias).astype(BF16).astype(F32)
        pn = ((side[0:1] - pmu) * pscale * gain + bias).astype(BF16).astype(F32)
        pn = jnp.where(live, pn, 0.0)
        prev = jnp.where(head, pn, pltpu.roll(xn, 1, 0))
        xk = (xn + (prev - xn) * blend).astype(BF16)
        if g * width % step == 0:
            copy(g * width // step).wait()
        acc = acc + dot(xk, w_ref[g * width : (g + 1) * width, 0:cut], NN)
    hidden = jnp.square(jnp.maximum(acc, 0.0))
    hidden = jnp.where(iota(hidden.shape, 1) < units, hidden, 0.0)
    hidden = pltpu.roll(hidden, 64, 1).astype(BF16)
    for g in range(groups):
        out = dot(hidden, w_ref[g * width : (g + 1) * width, units - 64 : wide], NT)
        out_ref[g] = out.astype(BF16)


VMEM = functools.partial(pl.BlockSpec, memory_space=pltpu.VMEM)
SMEM = functools.partial(pl.BlockSpec, memory_space=pltpu.SMEM)


def make(interpret):
    def call(kernel, outs, *args, in_specs=None, **more):
        return pl.pallas_call(
            kernel,
            out_shape=[jax.ShapeDtypeStruct(s, t) for s, t in outs],
            in_specs=in_specs or [VMEM() for _ in args],
            out_specs=[VMEM() for _ in outs],
            interpret=interpret,
            **more,
        )(*args)

    def local(
        skip, recept, keys, values, gating, logit, boost, gn_gain, gn_bias, ln_gain, ln_bias, blend, wk, wv
    ):
        rows, width = skip.shape
        groups = lax.axis_size("hid")
        blocks = lax.axis_size(SEQ)
        at_seq = lax.axis_index(SEQ).reshape(1)

        weights = lax.all_gather(jnp.concatenate([wk, wv], axis=1), SEQ, tiled=True)
        own, recall, state = call(
            wkv_kernel,
            [((rows, width), F32), ((rows, width), BF16), ((72, width), BF16)],
            recept, keys, values, logit, boost.reshape(1, width),
        )
        states = lax.all_to_all(
            jnp.broadcast_to(state, (blocks, *state.shape)), SEQ, 0, 0, tiled=True
        )
        middle, main, edge, vecs = call(
            middle_kernel,
            [((rows, width), F32), ((rows - 8, width), BF16), ((8, width), BF16), ((8, width), BF16)],
            at_seq, states, own, recall, skip, gating,
            jnp.stack([gn_gain, gn_bias]), jnp.stack([ln_gain, ln_bias, blend]),
            in_specs=[SMEM()] + [VMEM()] * 7,
        )
        before = lax.ppermute(edge, SEQ, [(n, n + 1) for n in range(blocks - 1)])
        side = jnp.stack([edge, jnp.concatenate([before[7:8], vecs[1:8]])])
        side = lax.all_to_all(
            jnp.broadcast_to(side, (groups, *side.shape)), "hid", 0, 0, tiled=True
        )
        main = lax.all_gather(main, "hid")
        (part,) = call(
            ffn_kernel,
            [((groups, rows, width), BF16)],
            at_seq, main, side, weights,
            in_specs=[SMEM(), VMEM(), VMEM(), pl.BlockSpec(memory_space=pl.ANY)],
            scratch_shapes=[pltpu.VMEM(weights.shape, BF16), pltpu.SemaphoreType.DMA((min(8, groups),))],
        )
        part = lax.all_to_all(part, "hid", 0, 0, tiled=True)
        return (middle + jnp.sum(part.astype(F32), axis=0)).astype(BF16)

    return local


def build(finer, interpret=False):
    tile, vec = P(SEQ, "hid"), P("hid")
    return jax.shard_map(
        make(interpret),
        mesh=finer,
        in_specs=(tile,) * 6 + (P("hid", None),) + (vec,) * 5 + (tile, tile),
        out_specs=tile,
        check_vma=False,
    )


def solution(mesh):
    return build(Mesh(mesh.devices.reshape(4, 4, 2, mesh.shape["hid"]), (*SEQ, "hid")))
```

```python
import functools

import jax
import jax.numpy as jnp
from jax import lax
from jax.experimental import pallas as pl
from jax.experimental.pallas import tpu as pltpu
from jax.sharding import Mesh
from jax.sharding import PartitionSpec as P

SEQ = ("y", "x", "c")
EPS_GROUP = 0.00064
EPS_LAYER = 1e-05
F32 = jnp.float32
BF16 = jnp.bfloat16
NN = (((1,), (0,)), ((), ()))
NT = (((1,), (1,)), ((), ()))
TN = (((0,), (0,)), ((), ()))


def dot(a, b, dims):
    return lax.dot_general(a, b, dims, preferred_element_type=F32)


def iota(shape, dim):
    return lax.broadcasted_iota(jnp.int32, shape, dim)


def hi_lo(x):
    hi = x.astype(BF16)
    return hi, (x - hi.astype(F32)).astype(BF16)


def wkv_kernel(r_ref, k_ref, v_ref, logit_ref, boost_ref, own_ref, rec_ref, pay_ref):
    rows, width = r_ref.shape
    logw = -jnp.exp(logit_ref[...])
    lower = (iota((rows, rows), 0) >= iota((rows, rows), 1)).astype(BF16)
    part0, rest = logw.astype(BF16), logw
    rest = rest - part0.astype(F32)
    part1, part2 = hi_lo(rest)
    incl = dot(lower, part0, NN) + dot(lower, part1, NN) + dot(lower, part2, NN)
    excl = incl - logw
    total = incl[rows - 1 : rows]
    half = rows // 2
    edge = incl[half - 1 : half]
    top = iota((rows, width), 0) < half
    ref = jnp.where(top, incl[half // 2 - 1 : half // 2], incl[half + half // 2 - 1 : half + half // 2])
    r = r_ref[...].astype(F32)
    k = k_ref[...].astype(F32)
    v = v_ref[...]
    r_in = (r * jnp.exp(excl - ref)).astype(BF16)
    k_in = (k * jnp.exp(ref - incl)).astype(BF16)
    r_off = (r * jnp.exp(jnp.minimum(excl - edge, 0.0))).astype(BF16)
    k_off = (k * jnp.exp(jnp.minimum(edge - incl, 0.0))).astype(BF16)
    rec_ref[...] = (r * jnp.exp(excl)).astype(BF16)
    k_end = (k * jnp.exp(total - incl)).astype(BF16)
    boost = jnp.concatenate([boost_ref[h : h + 1] for h in range(boost_ref.shape[0])], axis=1)
    now = r * boost * k
    row, col = iota((rows, rows), 0), iota((rows, rows), 1)
    same = (row > col) & ((row < half) == (col < half))
    cross = (row >= half) & (col < half)
    left = iota((rows, 128), 1) < 64
    zero = jnp.zeros((), BF16)
    for p in range(width // 128):
        at = slice(128 * p, 128 * p + 128)
        scores, values, sums = [], [], []
        for mask in (left, ~left):
            inner = dot(r_in[:, at], jnp.where(mask, k_in[:, at], zero), NT)
            outer = dot(r_off[:, at], jnp.where(mask, k_off[:, at], zero), NT)
            scores.append(jnp.where(same, inner, jnp.where(cross, outer, 0.0)).astype(BF16))
            values.append(jnp.where(mask, v[:, at], zero))
            sums.append(jnp.sum(jnp.where(mask, now[:, at], 0.0), axis=1, keepdims=True))
        out = dot(jnp.concatenate(scores, axis=1), jnp.concatenate(values, axis=0), NN)
        own_ref[:, at] = out + jnp.where(left, sums[0], sums[1]) * v[:, at].astype(F32)
        state = dot(v[:, at], k_end[:, at], TN)
        pay_ref[0:64, at] = jnp.where(left[0:64], state[0:64], state[64:128]).astype(BF16)
    hi, lo = hi_lo(total)
    line = iota((8, width), 0)
    pay_ref[64:72, :] = jnp.where(
        line == 0, hi.astype(F32), jnp.where(line == 1, lo.astype(F32), 0.0)
    ).astype(BF16)


def pair_kernel(pair_ref, wk_ref, wv_ref, out_ref, w_ref):
    units = wk_ref.shape[0]
    w_ref[0:units] = wk_ref[...]
    w_ref[units:] = wv_ref[...]
    a, b = pair_ref[0].astype(F32), pair_ref[1].astype(F32)
    last = b[64:65] + b[65:66]
    state = (a[0:64] * jnp.exp(last) + b[0:64]).astype(BF16)
    hi, lo = hi_lo(a[64:65] + a[65:66] + last)
    line = iota((8, a.shape[1]), 0)
    tail = jnp.where(line == 0, hi.astype(F32), jnp.where(line == 1, lo.astype(F32), 0.0)).astype(BF16)
    for n in range(out_ref.shape[0]):
        out_ref[n, 0:64] = state
        out_ref[n, 64:72] = tail


def middle_kernel(
    at_ref, all_ref, pair_ref, own_ref, rec_ref, skip_ref, gate_ref, gn_ref, ln_ref,
    mid_ref, main_ref, edge_ref, tile_ref,
):
    rows, width = own_ref.shape
    main = main_ref.shape[0]

    def join(ref):
        def step(i, state):
            piece = ref[i].astype(F32)
            return state * jnp.exp(piece[64:65] + piece[65:66]) + piece[0:64]

        return step

    state = lax.fori_loop(0, at_ref[0], join(all_ref), jnp.zeros((64, width), F32))
    state = lax.fori_loop(0, at_ref[1], join(pair_ref), state)
    left64 = iota((64, 128), 1) < 64
    left = iota((rows, 128), 1) < 64

    def mean(x):
        a = jnp.sum(jnp.where(left, x, 0.0), axis=1, keepdims=True)
        b = jnp.sum(jnp.where(left, 0.0, x), axis=1, keepdims=True)
        return jnp.where(left, a, b) * (1.0 / 64)

    for p in range(width // 128):
        at = slice(128 * p, 128 * p + 128)
        here = state[:, at]
        both = jnp.concatenate(
            [jnp.where(left64, here, 0.0), jnp.where(left64, 0.0, here)], axis=0
        ).astype(BF16)
        wkv = own_ref[:, at] + dot(rec_ref[:, at], both, NT)
        centre = wkv - mean(wkv)
        normed = centre * lax.rsqrt(mean(centre * centre) + EPS_GROUP)
        normed = normed * gn_ref[0:1, at] + gn_ref[1:2, at]
        gate = gate_ref[:, at].astype(F32)
        middle = skip_ref[:, at].astype(F32) + normed * (gate / (1.0 + jnp.exp(-gate)))
        mid_ref[:, at] = middle
        main_ref[:, at] = middle[0:main].astype(BF16)
        edge_ref[:, at] = middle[main:].astype(BF16)
    line = iota((8, width), 0)
    tail = jnp.where(line == 0, mid_ref[rows - 1 : rows, :], 0.0)
    for n in range(3):
        hi, lo = hi_lo(ln_ref[n : n + 1])
        tail = jnp.where(line == 2 * n + 1, hi.astype(F32), tail)
        tail = jnp.where(line == 2 * n + 2, lo.astype(F32), tail)
    tile_ref[...] = tail.astype(BF16)


def ffn_kernel(at_ref, main_ref, side_ref, w_hbm, out_ref, w_ref, sems):
    groups, rows, width = out_ref.shape
    main = main_ref.shape[1]
    full = groups * width
    depth = w_hbm.shape[1]
    tall = w_hbm.shape[0] // (full // depth)
    units = tall // 2
    chunks = sems.shape[0]
    step = full // chunks

    def copy(q):
        at = pl.ds(q * step // depth * tall, step // depth * tall)
        return pltpu.make_async_copy(w_hbm.at[at], w_ref.at[at], sems.at[q])

    def weights(g, first):
        blocks = range(g * width // depth, (g + 1) * width // depth)
        return jnp.concatenate([w_ref[b * tall + first : b * tall + first + units] for b in blocks], axis=1)

    for q in range(chunks):
        copy(q).start()

    def load(g):
        return jnp.concatenate([main_ref[g].astype(F32), side_ref[g, 0].astype(F32)], axis=0)

    def stats(get, n):
        first, second = jnp.zeros((n, width), F32), jnp.zeros((n, width), F32)
        for g in range(groups):
            x = get(g)
            first, second = first + x, second + x * x
        mu = jnp.sum(first, axis=1, keepdims=True) / full
        var = jnp.sum(second, axis=1, keepdims=True) / full - mu * mu
        return mu, lax.rsqrt(var + EPS_LAYER)

    mu, scale = stats(load, rows)
    pmu, pscale = stats(lambda g: side_ref[g, 1].astype(F32)[0:1], 1)
    live = at_ref[0] > 0
    head = iota((rows, width), 0) == 0
    acc = jnp.zeros((rows, units), F32)
    for g in range(groups):
        side = side_ref[g, 1].astype(F32)
        gain, bias, blend = (side[n : n + 1] + side[n + 1 : n + 2] for n in (1, 3, 5))
        xn = ((load(g) - mu) * scale * gain + bias).astype(BF16).astype(F32)
        pn = ((side[0:1] - pmu) * pscale * gain + bias).astype(BF16).astype(F32)
        pn = jnp.where(live, pn, 0.0)
        prev = jnp.where(head, pn, pltpu.roll(xn, 1, 0))
        xk = (xn + (prev - xn) * blend).astype(BF16)
        if g * width % step == 0:
            copy(g * width // step).wait()
        acc = acc + dot(xk, weights(g, 0), NT)
    hidden = jnp.square(jnp.maximum(acc, 0.0)).astype(BF16)
    for g in range(groups):
        out_ref[g] = dot(hidden, weights(g, units), NN).astype(BF16)


VMEM = functools.partial(pl.BlockSpec, memory_space=pltpu.VMEM)
SMEM = functools.partial(pl.BlockSpec, memory_space=pltpu.SMEM)


def make(interpret):
    def call(kernel, outs, *args, in_specs=None, **more):
        return pl.pallas_call(
            kernel,
            out_shape=[jax.ShapeDtypeStruct(s, t) for s, t in outs],
            in_specs=in_specs or [VMEM() for _ in args],
            out_specs=[VMEM() for _ in outs],
            interpret=interpret,
            **more,
        )(*args)

    def local(
        skip, recept, keys, values, gating, logit, boost, gn_gain, gn_bias, ln_gain, ln_bias, blend, wk, wv
    ):
        rows, width = skip.shape
        groups = lax.axis_size("hid")
        blocks = lax.axis_size(SEQ)
        at_seq = lax.axis_index(SEQ).reshape(1)

        core = lax.axis_index("c")
        chips = blocks // lax.axis_size("c")
        own, recall, state = call(
            wkv_kernel,
            [((rows, width), F32), ((rows, width), BF16), ((72, width), BF16)],
            recept, keys, values, logit, boost,
        )
        pair = lax.all_gather(state, "c")
        states, weights = call(
            pair_kernel,
            [((chips, 72, width), BF16), ((2 * wk.shape[1], wk.shape[0]), BF16)],
            pair, wk.T, wv.T,
        )
        weights = lax.all_gather(weights, SEQ, tiled=True)
        states = lax.all_to_all(states, ("y", "x"), 0, 0, tiled=True)
        middle, main, edge, tile = call(
            middle_kernel,
            [((rows, width), F32), ((rows - 8, width), BF16), ((8, width), BF16), ((8, width), BF16)],
            jnp.stack([lax.axis_index(("y", "x")), core]),
            states, pair, own, recall, skip, gating,
            jnp.stack([gn_gain, gn_bias]), jnp.stack([ln_gain, ln_bias, blend]),
            in_specs=[SMEM()] + [VMEM()] * 8,
        )
        tile = lax.ppermute(tile, SEQ, [(n, (n + 1) % blocks) for n in range(blocks)])
        side = jnp.stack([edge, tile])
        side = lax.all_to_all(
            jnp.broadcast_to(side, (groups, *side.shape)), "hid", 0, 0, tiled=True
        )
        main = lax.all_gather(main, "hid")
        (part,) = call(
            ffn_kernel,
            [((groups, rows, width), BF16)],
            at_seq, main, side, weights,
            in_specs=[SMEM(), VMEM(), VMEM(), pl.BlockSpec(memory_space=pl.ANY)],
            scratch_shapes=[pltpu.VMEM(weights.shape, BF16), pltpu.SemaphoreType.DMA((min(8, groups),))],
        )
        part = lax.all_to_all(part, "hid", 0, 0, tiled=True)
        return (middle + jnp.sum(part.astype(F32), axis=0)).astype(BF16)

    return local


def build(finer, interpret=False):
    tile, vec = P(SEQ, "hid"), P("hid")
    return jax.shard_map(
        make(interpret),
        mesh=finer,
        in_specs=(tile,) * 6 + (P("hid", None),) + (vec,) * 5 + (tile, tile),
        out_specs=tile,
        check_vma=False,
    )


def solution(mesh):
    return build(Mesh(mesh.devices.reshape(4, 4, 2, mesh.shape["hid"]), (*SEQ, "hid")))
```

```python
import functools

import jax
import jax.numpy as jnp
from jax import lax
from jax.experimental import pallas as pl
from jax.experimental.pallas import tpu as pltpu
from jax.sharding import Mesh
from jax.sharding import PartitionSpec as P

SEQ = ("y", "x", "c")
EPS_GROUP = 0.00064
EPS_LAYER = 1e-05
F32 = jnp.float32
BF16 = jnp.bfloat16
NN = (((1,), (0,)), ((), ()))
NT = (((1,), (1,)), ((), ()))
TN = (((0,), (0,)), ((), ()))


def dot(a, b, dims):
    return lax.dot_general(a, b, dims, preferred_element_type=F32)


def iota(shape, dim):
    return lax.broadcasted_iota(jnp.int32, shape, dim)


def hi_lo(x):
    hi = x.astype(BF16)
    return hi, (x - hi.astype(F32)).astype(BF16)


def last_row(ref):
    rows = ref.shape[0]
    return ref[rows - 16 : rows, :].astype(F32)[15:16]


def wkv_kernel(
    r_ref, k_ref, v_ref, logit_ref, boost_ref, skip_ref, gate_ref, own_ref, rec_ref, pay_ref, row_ref
):
    rows, width = r_ref.shape
    logw = -jnp.exp(logit_ref[...])
    lower = (iota((rows, rows), 0) >= iota((rows, rows), 1)).astype(BF16)
    part0, rest = logw.astype(BF16), logw
    rest = rest - part0.astype(F32)
    part1, part2 = hi_lo(rest)
    incl = dot(lower, part0, NN) + dot(lower, part1, NN) + dot(lower, part2, NN)
    excl = incl - logw
    total = incl[rows - 1 : rows]
    half = rows // 2
    edge = incl[half - 1 : half]
    top = iota((rows, width), 0) < half
    ref = jnp.where(top, incl[half // 2 - 1 : half // 2], incl[half + half // 2 - 1 : half + half // 2])
    r = r_ref[...].astype(F32)
    k = k_ref[...].astype(F32)
    v = v_ref[...]
    r_in = (r * jnp.exp(excl - ref)).astype(BF16)
    k_in = (k * jnp.exp(ref - incl)).astype(BF16)
    r_off = (r * jnp.exp(jnp.minimum(excl - edge, 0.0))).astype(BF16)
    k_off = (k * jnp.exp(jnp.minimum(edge - incl, 0.0))).astype(BF16)
    rec_ref[...] = (r * jnp.exp(excl)).astype(BF16)
    k_end = (k * jnp.exp(total - incl)).astype(BF16)
    boost = jnp.concatenate([boost_ref[h : h + 1] for h in range(boost_ref.shape[0])], axis=1)
    now = r * boost * k
    row, col = iota((rows, rows), 0), iota((rows, rows), 1)
    same = (row > col) & ((row < half) == (col < half))
    cross = (row >= half) & (col < half)
    left = iota((rows, 128), 1) < 64
    zero = jnp.zeros((), BF16)
    for p in range(width // 128):
        at = slice(128 * p, 128 * p + 128)
        scores, values, sums = [], [], []
        for mask in (left, ~left):
            inner = dot(r_in[:, at], jnp.where(mask, k_in[:, at], zero), NT)
            outer = dot(r_off[:, at], jnp.where(mask, k_off[:, at], zero), NT)
            scores.append(jnp.where(same, inner, jnp.where(cross, outer, 0.0)).astype(BF16))
            values.append(jnp.where(mask, v[:, at], zero))
            sums.append(jnp.sum(jnp.where(mask, now[:, at], 0.0), axis=1, keepdims=True))
        out = dot(jnp.concatenate(scores, axis=1), jnp.concatenate(values, axis=0), NN)
        own_ref[:, at] = out + jnp.where(left, sums[0], sums[1]) * v[:, at].astype(F32)
        state = dot(v[:, at], k_end[:, at], TN)
        pay_ref[0:64, at] = jnp.where(left[0:64], state[0:64], state[64:128]).astype(BF16)
    hi, lo = hi_lo(total)
    line = iota((8, width), 0)
    pay_ref[64:72, :] = jnp.where(
        line == 0, hi.astype(F32), jnp.where(line == 1, lo.astype(F32), 0.0)
    ).astype(BF16)
    tail = jnp.where(line == 0, last_row(own_ref), 0.0)
    tail = jnp.where(line == 1, last_row(rec_ref), tail)
    tail = jnp.where(line == 2, last_row(skip_ref), tail)
    row_ref[...] = jnp.where(line == 3, last_row(gate_ref), tail)


def apart(state, at):
    left = iota((64, 128), 1) < 64
    here = state[:, at]
    both = [jnp.where(left, here, 0.0), jnp.where(left, 0.0, here)]
    return jnp.concatenate(both, axis=0).astype(BF16)


def pair_kernel(at_ref, pair_ref, row_ref, wk_ref, wv_ref, out_ref, send_ref, w_ref):
    units = wk_ref.shape[0]
    w_ref[0:units] = wk_ref[...]
    w_ref[units:] = wv_ref[...]
    a, b = pair_ref[0].astype(F32), pair_ref[1].astype(F32)
    last = b[64:65] + b[65:66]
    state = (a[0:64] * jnp.exp(last) + b[0:64]).astype(BF16)
    hi, lo = hi_lo(a[64:65] + a[65:66] + last)
    line = iota((8, a.shape[1]), 0)
    tail = jnp.where(line == 0, hi.astype(F32), jnp.where(line == 1, lo.astype(F32), 0.0)).astype(BF16)
    for n in range(out_ref.shape[0]):
        out_ref[n, 0:64] = state
        out_ref[n, 64:72] = tail
    second = at_ref[1] > 0
    row = row_ref[...]
    for p in range(a.shape[1] // 128):
        at = slice(128 * p, 128 * p + 128)
        recall = row[1:2, at]
        more = dot(jnp.broadcast_to(recall, (8, 128)).astype(BF16), apart(a[0:64], at), NT)
        fade = recall * (jnp.exp(a[64:65, at] + a[65:66, at]) - 1.0)
        more = jnp.where(line[:, at] == 0, more, jnp.where(line[:, at] == 1, fade, 0.0))
        send_ref[:, at] = row[:, at] + jnp.where(second, more, 0.0)


def middle_kernel(
    at_ref, all_ref, pair_ref, prior_ref, own_ref, rec_ref, skip_ref, gate_ref, gn_ref, ln_ref,
    mid_ref, main_ref, side_ref,
):
    rows, width = own_ref.shape
    main = main_ref.shape[0]

    def join(ref):
        def step(i, state):
            piece = ref[i].astype(F32)
            return state * jnp.exp(piece[64:65] + piece[65:66]) + piece[0:64]

        return step

    chip, core = at_ref[0], at_ref[1]
    split = jnp.maximum(chip + core - 1, 0)
    old = lax.fori_loop(0, split, join(all_ref), jnp.zeros((64, width), F32))
    state = lax.fori_loop(split, chip, join(all_ref), old)
    state = lax.fori_loop(0, core, join(pair_ref), state)

    def finish(own, recall, skip, gate, before, at):
        left = iota(own.shape, 1) < 64

        def mean(x):
            a = jnp.sum(jnp.where(left, x, 0.0), axis=1, keepdims=True)
            b = jnp.sum(jnp.where(left, 0.0, x), axis=1, keepdims=True)
            return jnp.where(left, a, b) * (1.0 / 64)

        wkv = own + dot(recall, apart(before, at), NT)
        centre = wkv - mean(wkv)
        normed = centre * lax.rsqrt(mean(centre * centre) + EPS_GROUP)
        normed = normed * gn_ref[0:1, at] + gn_ref[1:2, at]
        return skip + normed * (gate / (1.0 + jnp.exp(-gate)))

    line = iota((8, 128), 0)
    for p in range(width // 128):
        at = slice(128 * p, 128 * p + 128)
        middle = finish(
            own_ref[:, at], rec_ref[:, at], skip_ref[:, at].astype(F32), gate_ref[:, at].astype(F32), state, at
        )
        mid_ref[:, at] = middle
        main_ref[:, at] = middle[0:main].astype(BF16)
        own, recall, skip, gate = (jnp.broadcast_to(prior_ref[n : n + 1, at], (8, 128)) for n in range(4))
        tail = jnp.where(line == 0, finish(own, recall.astype(BF16), skip, gate, old, at), 0.0)
        for n in range(3):
            hi, lo = hi_lo(ln_ref[n : n + 1, at])
            tail = jnp.where(line == 2 * n + 1, hi.astype(F32), tail)
            tail = jnp.where(line == 2 * n + 2, lo.astype(F32), tail)
        edge, tail = middle[main:].astype(BF16), tail.astype(BF16)
        for g in range(side_ref.shape[0]):
            side_ref[g, 0, :, at] = edge
            side_ref[g, 1, :, at] = tail


def ffn_kernel(at_ref, main_ref, side_ref, w_hbm, out_ref, w_ref, sems):
    groups, rows, width = out_ref.shape
    main = main_ref.shape[1]
    full = groups * width
    depth = w_hbm.shape[1]
    tall = w_hbm.shape[0] // (full // depth)
    units = tall // 2
    chunks = sems.shape[0]
    step = full // chunks

    def copy(q):
        at = pl.ds(q * step // depth * tall, step // depth * tall)
        return pltpu.make_async_copy(w_hbm.at[at], w_ref.at[at], sems.at[q])

    def weights(g, first):
        blocks = range(g * width // depth, (g + 1) * width // depth)
        return jnp.concatenate([w_ref[b * tall + first : b * tall + first + units] for b in blocks], axis=1)

    for q in range(chunks):
        copy(q).start()

    def load(g):
        return jnp.concatenate([main_ref[g].astype(F32), side_ref[g, 0].astype(F32)], axis=0)

    def stats(get, n):
        first, second = jnp.zeros((n, width), F32), jnp.zeros((n, width), F32)
        for g in range(groups):
            x = get(g)
            first, second = first + x, second + x * x
        mu = jnp.sum(first, axis=1, keepdims=True) / full
        var = jnp.sum(second, axis=1, keepdims=True) / full - mu * mu
        return mu, lax.rsqrt(var + EPS_LAYER)

    mu, scale = stats(load, rows)
    pmu, pscale = stats(lambda g: side_ref[g, 1].astype(F32)[0:1], 1)
    live = at_ref[0] > 0
    head = iota((rows, width), 0) == 0
    acc = jnp.zeros((rows, units), F32)
    for g in range(groups):
        side = side_ref[g, 1].astype(F32)
        gain, bias, blend = (side[n : n + 1] + side[n + 1 : n + 2] for n in (1, 3, 5))
        xn = ((load(g) - mu) * scale * gain + bias).astype(BF16).astype(F32)
        pn = ((side[0:1] - pmu) * pscale * gain + bias).astype(BF16).astype(F32)
        pn = jnp.where(live, pn, 0.0)
        prev = jnp.where(head, pn, pltpu.roll(xn, 1, 0))
        xk = (xn + (prev - xn) * blend).astype(BF16)
        if g * width % step == 0:
            copy(g * width // step).wait()
        acc = acc + dot(xk, weights(g, 0), NT)
    hidden = jnp.square(jnp.maximum(acc, 0.0)).astype(BF16)
    for g in range(groups):
        out_ref[g] = dot(hidden, weights(g, units), NN).astype(BF16)


VMEM = functools.partial(pl.BlockSpec, memory_space=pltpu.VMEM)
SMEM = functools.partial(pl.BlockSpec, memory_space=pltpu.SMEM)


def make(interpret):
    def call(kernel, outs, *args, in_specs=None, **more):
        return pl.pallas_call(
            kernel,
            out_shape=[jax.ShapeDtypeStruct(s, t) for s, t in outs],
            in_specs=in_specs or [VMEM() for _ in args],
            out_specs=[VMEM() for _ in outs],
            interpret=interpret,
            **more,
        )(*args)

    def local(
        skip, recept, keys, values, gating, logit, boost, gn_gain, gn_bias, ln_gain, ln_bias, blend, wk, wv
    ):
        rows, width = skip.shape
        groups = lax.axis_size("hid")
        blocks = lax.axis_size(SEQ)
        at_seq = lax.axis_index(SEQ).reshape(1)

        core = lax.axis_index("c")
        chips = blocks // lax.axis_size("c")
        at = jnp.stack([lax.axis_index(("y", "x")), core])
        own, recall, state, row = call(
            wkv_kernel,
            [((rows, width), F32), ((rows, width), BF16), ((72, width), BF16), ((8, width), F32)],
            recept, keys, values, logit, boost, skip, gating,
        )
        pair = lax.all_gather(state, "c")
        states, row, weights = call(
            pair_kernel,
            [((chips, 72, width), BF16), ((8, width), F32), ((2 * wk.shape[1], wk.shape[0]), BF16)],
            at, pair, row, wk.T, wv.T,
            in_specs=[SMEM()] + [VMEM()] * 4,
        )
        weights = lax.all_gather(weights, SEQ, tiled=True)
        states = lax.all_to_all(states, ("y", "x"), 0, 0, tiled=True)
        prior = lax.ppermute(row, SEQ, [(n, n + 1) for n in range(blocks - 1)])
        middle, main, side = call(
            middle_kernel,
            [((rows, width), F32), ((rows - 8, width), BF16), ((groups, 2, 8, width), BF16)],
            at, states, pair, prior, own, recall, skip, gating,
            jnp.stack([gn_gain, gn_bias]), jnp.stack([ln_gain, ln_bias, blend]),
            in_specs=[SMEM()] + [VMEM()] * 9,
        )
        side = lax.all_to_all(side, "hid", 0, 0, tiled=True)
        main = lax.all_gather(main, "hid")
        (part,) = call(
            ffn_kernel,
            [((groups, rows, width), BF16)],
            at_seq, main, side, weights,
            in_specs=[SMEM(), VMEM(), VMEM(), pl.BlockSpec(memory_space=pl.ANY)],
            scratch_shapes=[pltpu.VMEM(weights.shape, BF16), pltpu.SemaphoreType.DMA((min(8, groups),))],
        )
        part = lax.all_to_all(part, "hid", 0, 0, tiled=True)
        return (middle + jnp.sum(part.astype(F32), axis=0)).astype(BF16)

    return local


def build(finer, interpret=False):
    tile, vec = P(SEQ, "hid"), P("hid")
    return jax.shard_map(
        make(interpret),
        mesh=finer,
        in_specs=(tile,) * 6 + (P("hid", None),) + (vec,) * 5 + (tile, tile),
        out_specs=tile,
        check_vma=False,
    )


def solution(mesh):
    return build(Mesh(mesh.devices.reshape(4, 4, 2, mesh.shape["hid"]), (*SEQ, "hid")))
```

```python
import functools

import jax
import jax.numpy as jnp
from jax import lax
from jax.experimental import pallas as pl
from jax.experimental.pallas import tpu as pltpu
from jax.sharding import Mesh
from jax.sharding import PartitionSpec as P

SEQ = ("y", "x", "c")
HID = ("zl", "zh")
EPS_GROUP = 0.00064
EPS_LAYER = 1e-05
F32 = jnp.float32
BF16 = jnp.bfloat16
NN = (((1,), (0,)), ((), ()))
NT = (((1,), (1,)), ((), ()))
TN = (((0,), (0,)), ((), ()))


def dot(a, b, dims):
    return lax.dot_general(a, b, dims, preferred_element_type=F32)


def iota(shape, dim):
    return lax.broadcasted_iota(jnp.int32, shape, dim)


def hi_lo(x):
    hi = x.astype(BF16)
    return hi, (x - hi.astype(F32)).astype(BF16)


def last_row(ref):
    rows = ref.shape[0]
    return ref[rows - 16 : rows, :].astype(F32)[15:16]


def wkv_kernel(
    r_ref, k_ref, v_ref, logit_ref, boost_ref, skip_ref, gate_ref, own_ref, rec_ref, pay_ref, row_ref
):
    rows, width = r_ref.shape
    logw = -jnp.exp(logit_ref[...])
    lower = (iota((rows, rows), 0) >= iota((rows, rows), 1)).astype(BF16)
    part0, rest = logw.astype(BF16), logw
    rest = rest - part0.astype(F32)
    part1, part2 = hi_lo(rest)
    incl = dot(lower, part0, NN) + dot(lower, part1, NN) + dot(lower, part2, NN)
    excl = incl - logw
    total = incl[rows - 1 : rows]
    half = rows // 2
    edge = incl[half - 1 : half]
    top = iota((rows, width), 0) < half
    ref = jnp.where(top, incl[half // 2 - 1 : half // 2], incl[half + half // 2 - 1 : half + half // 2])
    r = r_ref[...].astype(F32)
    k = k_ref[...].astype(F32)
    v = v_ref[...]
    r_in = (r * jnp.exp(excl - ref)).astype(BF16)
    k_in = (k * jnp.exp(ref - incl)).astype(BF16)
    r_off = (r * jnp.exp(jnp.minimum(excl - edge, 0.0))).astype(BF16)
    k_off = (k * jnp.exp(jnp.minimum(edge - incl, 0.0))).astype(BF16)
    rec_ref[...] = (r * jnp.exp(excl)).astype(BF16)
    k_end = (k * jnp.exp(total - incl)).astype(BF16)
    boost = jnp.concatenate([boost_ref[h : h + 1] for h in range(boost_ref.shape[0])], axis=1)
    now = r * boost * k
    row, col = iota((rows, rows), 0), iota((rows, rows), 1)
    same = (row > col) & ((row < half) == (col < half))
    cross = (row >= half) & (col < half)
    left = iota((rows, 128), 1) < 64
    zero = jnp.zeros((), BF16)
    for p in range(width // 128):
        at = slice(128 * p, 128 * p + 128)
        scores, values, sums = [], [], []
        for mask in (left, ~left):
            inner = dot(r_in[:, at], jnp.where(mask, k_in[:, at], zero), NT)
            outer = dot(r_off[:, at], jnp.where(mask, k_off[:, at], zero), NT)
            scores.append(jnp.where(same, inner, jnp.where(cross, outer, 0.0)).astype(BF16))
            values.append(jnp.where(mask, v[:, at], zero))
            sums.append(jnp.sum(jnp.where(mask, now[:, at], 0.0), axis=1, keepdims=True))
        out = dot(jnp.concatenate(scores, axis=1), jnp.concatenate(values, axis=0), NN)
        own_ref[:, at] = out + jnp.where(left, sums[0], sums[1]) * v[:, at].astype(F32)
        state = dot(v[:, at], k_end[:, at], TN)
        pay_ref[0:64, at] = jnp.where(left[0:64], state[0:64], state[64:128]).astype(BF16)
    hi, lo = hi_lo(total)
    line = iota((8, width), 0)
    pay_ref[64:72, :] = jnp.where(
        line == 0, hi.astype(F32), jnp.where(line == 1, lo.astype(F32), 0.0)
    ).astype(BF16)
    tail = jnp.where(line == 0, last_row(own_ref), 0.0)
    tail = jnp.where(line == 1, last_row(rec_ref), tail)
    tail = jnp.where(line == 2, last_row(skip_ref), tail)
    row_ref[...] = jnp.where(line == 3, last_row(gate_ref), tail)


def apart(state, at):
    left = iota((64, 128), 1) < 64
    here = state[:, at]
    both = [jnp.where(left, here, 0.0), jnp.where(left, 0.0, here)]
    return jnp.concatenate(both, axis=0).astype(BF16)


def pair_kernel(at_ref, pair_ref, row_ref, wk_ref, wv_ref, out_ref, send_ref, w_ref):
    units = wk_ref.shape[0]
    w_ref[0:units] = wk_ref[...]
    w_ref[units:] = wv_ref[...]
    a, b = pair_ref[0].astype(F32), pair_ref[1].astype(F32)
    last = b[64:65] + b[65:66]
    state = (a[0:64] * jnp.exp(last) + b[0:64]).astype(BF16)
    hi, lo = hi_lo(a[64:65] + a[65:66] + last)
    line = iota((8, a.shape[1]), 0)
    tail = jnp.where(line == 0, hi.astype(F32), jnp.where(line == 1, lo.astype(F32), 0.0)).astype(BF16)
    for n in range(out_ref.shape[0]):
        out_ref[n, 0:64] = state
        out_ref[n, 64:72] = tail
    second = at_ref[1] > 0
    row = row_ref[...]
    for p in range(a.shape[1] // 128):
        at = slice(128 * p, 128 * p + 128)
        recall = row[1:2, at]
        more = dot(jnp.broadcast_to(recall, (8, 128)).astype(BF16), apart(a[0:64], at), NT)
        fade = recall * (jnp.exp(a[64:65, at] + a[65:66, at]) - 1.0)
        more = jnp.where(line[:, at] == 0, more, jnp.where(line[:, at] == 1, fade, 0.0))
        send_ref[:, at] = row[:, at] + jnp.where(second, more, 0.0)


def middle_kernel(
    at_ref, all_ref, pair_ref, prior_ref, own_ref, rec_ref, skip_ref, gate_ref, gn_ref, ln_ref,
    mid_ref, main_ref, side_ref,
):
    rows, width = own_ref.shape
    main = main_ref.shape[0]

    def join(ref):
        def step(i, state):
            piece = ref[i].astype(F32)
            return state * jnp.exp(piece[64:65] + piece[65:66]) + piece[0:64]

        return step

    chip, core = at_ref[0], at_ref[1]
    split = jnp.maximum(chip + core - 1, 0)
    old = lax.fori_loop(0, split, join(all_ref), jnp.zeros((64, width), F32))
    state = lax.fori_loop(split, chip, join(all_ref), old)
    state = lax.fori_loop(0, core, join(pair_ref), state)

    def finish(own, recall, skip, gate, before, at):
        left = iota(own.shape, 1) < 64

        def mean(x):
            a = jnp.sum(jnp.where(left, x, 0.0), axis=1, keepdims=True)
            b = jnp.sum(jnp.where(left, 0.0, x), axis=1, keepdims=True)
            return jnp.where(left, a, b) * (1.0 / 64)

        wkv = own + dot(recall, apart(before, at), NT)
        centre = wkv - mean(wkv)
        normed = centre * lax.rsqrt(mean(centre * centre) + EPS_GROUP)
        normed = normed * gn_ref[0:1, at] + gn_ref[1:2, at]
        return skip + normed * (gate / (1.0 + jnp.exp(-gate)))

    line = iota((8, 128), 0)
    for p in range(width // 128):
        at = slice(128 * p, 128 * p + 128)
        middle = finish(
            own_ref[:, at], rec_ref[:, at], skip_ref[:, at].astype(F32), gate_ref[:, at].astype(F32), state, at
        )
        mid_ref[:, at] = middle
        main_ref[:, at] = middle[0:main].astype(BF16)
        own, recall, skip, gate = (jnp.broadcast_to(prior_ref[n : n + 1, at], (8, 128)) for n in range(4))
        tail = jnp.where(line == 0, finish(own, recall.astype(BF16), skip, gate, old, at), 0.0)
        for n in range(3):
            hi, lo = hi_lo(ln_ref[n : n + 1, at])
            tail = jnp.where(line == 2 * n + 1, hi.astype(F32), tail)
            tail = jnp.where(line == 2 * n + 2, lo.astype(F32), tail)
        edge, tail = middle[main:].astype(BF16), tail.astype(BF16)
        for g in range(side_ref.shape[0]):
            side_ref[g, 0, :, at] = edge
            side_ref[g, 1, :, at] = tail


def ffn_kernel(at_ref, main_ref, side_ref, w_hbm, give_ref, hidden_ref, w_ref, sems):
    _, rows, width = give_ref.shape
    groups, main = main_ref.shape[0:2]
    full = groups * width
    depth = w_hbm.shape[1]
    tall = w_hbm.shape[0] // (full // depth)
    units = tall // 2
    chunks = sems.shape[0]
    step = full // chunks

    def copy(q):
        at = pl.ds(q * step // depth * tall, step // depth * tall)
        return pltpu.make_async_copy(w_hbm.at[at], w_ref.at[at], sems.at[q])

    def weights(g, first):
        starts = [(g * (width // depth) + b) * tall + first for b in range(width // depth)]
        if not isinstance(g, int):
            starts = [pl.multiple_of(start, 64) for start in starts]
        return jnp.concatenate([w_ref[pl.ds(start, units)] for start in starts], axis=1)

    for q in range(chunks):
        copy(q).start()

    def load(g):
        return jnp.concatenate([main_ref[g].astype(F32), side_ref[g, 0].astype(F32)], axis=0)

    def stats(get, n):
        first, second = jnp.zeros((n, width), F32), jnp.zeros((n, width), F32)
        for g in range(groups):
            x = get(g)
            first, second = first + x, second + x * x
        mu = jnp.sum(first, axis=1, keepdims=True) / full
        var = jnp.sum(second, axis=1, keepdims=True) / full - mu * mu
        return mu, lax.rsqrt(var + EPS_LAYER)

    mu, scale = stats(load, rows)
    pmu, pscale = stats(lambda g: side_ref[g, 1].astype(F32)[0:1], 1)
    live = at_ref[0] > 0
    head = iota((rows, width), 0) == 0
    acc = jnp.zeros((rows, units), F32)
    for g in range(groups):
        side = side_ref[g, 1].astype(F32)
        gain, bias, blend = (side[n : n + 1] + side[n + 1 : n + 2] for n in (1, 3, 5))
        xn = ((load(g) - mu) * scale * gain + bias).astype(BF16).astype(F32)
        pn = ((side[0:1] - pmu) * pscale * gain + bias).astype(BF16).astype(F32)
        pn = jnp.where(live, pn, 0.0)
        prev = jnp.where(head, pn, pltpu.roll(xn, 1, 0))
        xk = (xn + (prev - xn) * blend).astype(BF16)
        if g * width % step == 0:
            copy(g * width // step).wait()
        acc = acc + dot(xk, weights(g, 0), NT)
    hidden = jnp.square(jnp.maximum(acc, 0.0)).astype(BF16)
    hidden_ref[...] = hidden
    for g in range(groups // 2):
        give_ref[g] = dot(hidden, weights(2 * g + 1 - at_ref[1], units), NN).astype(BF16)


def keep_kernel(at_ref, hidden_ref, w_hbm, keep_ref, w_ref, sems):
    groups, rows, width = keep_ref.shape
    units = hidden_ref.shape[1]
    depth = w_hbm.shape[1]
    each = width // depth

    def copy(g, b):
        start = (((2 * g + at_ref[1]) * each + b) * 2 + 1) * units
        return pltpu.make_async_copy(
            w_hbm.at[pl.ds(pl.multiple_of(start, 64), units)], w_ref.at[g * each + b], sems.at[g * each + b]
        )

    for g in range(groups):
        for b in range(each):
            copy(g, b).start()
    for g in range(groups):
        for b in range(each):
            copy(g, b).wait()
        w = jnp.concatenate([w_ref[g * each + b] for b in range(each)], axis=1)
        keep_ref[g] = dot(hidden_ref[...], w, NN).astype(BF16)


VMEM = functools.partial(pl.BlockSpec, memory_space=pltpu.VMEM)
SMEM = functools.partial(pl.BlockSpec, memory_space=pltpu.SMEM)


def make(interpret):
    def call(kernel, outs, *args, in_specs=None, **more):
        return pl.pallas_call(
            kernel,
            out_shape=[jax.ShapeDtypeStruct(s, t) for s, t in outs],
            in_specs=in_specs or [VMEM() for _ in args],
            out_specs=[VMEM() for _ in outs],
            interpret=interpret,
            **more,
        )(*args)

    def local(
        skip, recept, keys, values, gating, logit, boost, gn_gain, gn_bias, ln_gain, ln_bias, blend, wk, wv
    ):
        rows, width = skip.shape
        groups = lax.axis_size(HID)
        blocks = lax.axis_size(SEQ)
        at_seq = lax.axis_index(SEQ)

        core = lax.axis_index("c")
        chips = blocks // lax.axis_size("c")
        at = jnp.stack([lax.axis_index(("y", "x")), core])
        own, recall, state, row = call(
            wkv_kernel,
            [((rows, width), F32), ((rows, width), BF16), ((72, width), BF16), ((8, width), F32)],
            recept, keys, values, logit, boost, skip, gating,
        )
        pair = lax.all_gather(state, "c")
        states, row, weights = call(
            pair_kernel,
            [((chips, 72, width), BF16), ((8, width), F32), ((2 * wk.shape[1], wk.shape[0]), BF16)],
            at, pair, row, wk.T, wv.T,
            in_specs=[SMEM()] + [VMEM()] * 4,
        )
        weights = lax.all_gather(weights, SEQ, tiled=True)
        states = lax.all_to_all(states, ("y", "x"), 0, 0, tiled=True)
        prior = lax.ppermute(row, SEQ, [(n, n + 1) for n in range(blocks - 1)])
        middle, main, side = call(
            middle_kernel,
            [((rows, width), F32), ((rows - 8, width), BF16), ((groups, 2, 8, width), BF16)],
            at, states, pair, prior, own, recall, skip, gating,
            jnp.stack([gn_gain, gn_bias]), jnp.stack([ln_gain, ln_bias, blend]),
            in_specs=[SMEM()] + [VMEM()] * 9,
        )
        side = lax.all_to_all(side, HID, 0, 0, tiled=True)
        main = lax.all_gather(main, HID)
        at = jnp.stack([at_seq, lax.axis_index("zh")])
        any_space = pl.BlockSpec(memory_space=pl.ANY)
        units, depth = wk.shape[1], wk.shape[0]
        give, hidden = call(
            ffn_kernel,
            [((groups // 2, rows, width), BF16), ((rows, units), BF16)],
            at, main, side, weights,
            in_specs=[SMEM(), VMEM(), VMEM(), any_space],
            scratch_shapes=[pltpu.VMEM(weights.shape, BF16), pltpu.SemaphoreType.DMA((min(8, groups),))],
        )
        give = lax.ppermute(give, "zh", [(0, 1), (1, 0)])
        (keep,) = call(
            keep_kernel,
            [((groups // 2, rows, width), BF16)],
            at, hidden, weights,
            in_specs=[SMEM(), VMEM(), any_space],
            scratch_shapes=[pltpu.VMEM((blocks // 2, units, depth), BF16), pltpu.SemaphoreType.DMA((blocks // 2,))],
        )
        part = (keep.astype(F32) + give.astype(F32)).astype(BF16)
        part = lax.all_to_all(part, "zl", 0, 0, tiled=True)
        return (middle + jnp.sum(part.astype(F32), axis=0)).astype(BF16)

    return local


def build(finer, interpret=False):
    tile, vec = P(SEQ, HID), P(HID)
    return jax.shard_map(
        make(interpret),
        mesh=finer,
        in_specs=(tile,) * 6 + (P(HID, None),) + (vec,) * 5 + (tile, tile),
        out_specs=tile,
        check_vma=False,
    )


def solution(mesh):
    return build(Mesh(mesh.devices.reshape(4, 4, 2, mesh.shape["hid"] // 2, 2), (*SEQ, *HID)))
```

```python
import functools

import jax
import jax.numpy as jnp
from jax import lax
from jax.experimental import pallas as pl
from jax.experimental.pallas import tpu as pltpu
from jax.sharding import Mesh
from jax.sharding import PartitionSpec as P

SEQ = ("y", "x", "c")
HID = ("zl", "zh")
EPS_GROUP = 0.00064
EPS_LAYER = 1e-05
F32 = jnp.float32
BF16 = jnp.bfloat16
NN = (((1,), (0,)), ((), ()))
NT = (((1,), (1,)), ((), ()))
TN = (((0,), (0,)), ((), ()))


def dot(a, b, dims):
    return lax.dot_general(a, b, dims, preferred_element_type=F32)


def iota(shape, dim):
    return lax.broadcasted_iota(jnp.int32, shape, dim)


def hi_lo(x):
    hi = x.astype(BF16)
    return hi, (x - hi.astype(F32)).astype(BF16)


def last_row(ref):
    rows = ref.shape[0]
    return ref[rows - 16 : rows, :].astype(F32)[15:16]


def lines(*rows):
    width = rows[0].shape[1]
    line = iota((8, width), 0)
    tile = jnp.zeros((8, width), F32)
    for n, row in enumerate(rows):
        tile = jnp.where(line == n, row.astype(F32), tile)
    return tile.astype(BF16)


def wkv_kernel(
    r_ref, k_ref, v_ref, logit_ref, boost_ref, skip_ref, gate_ref, wk_ref, wv_ref,
    own_ref, rec_ref, pay_ref, w_ref,
):
    units = wk_ref.shape[0]
    w_ref[0:units] = wk_ref[...]
    w_ref[units:] = wv_ref[...]
    rows, width = r_ref.shape
    logw = -jnp.exp(logit_ref[...])
    lower = (iota((rows, rows), 0) >= iota((rows, rows), 1)).astype(BF16)
    part0, rest = logw.astype(BF16), logw
    rest = rest - part0.astype(F32)
    part1, part2 = hi_lo(rest)
    incl = dot(lower, part0, NN) + dot(lower, part1, NN) + dot(lower, part2, NN)
    excl = incl - logw
    total = incl[rows - 1 : rows]
    half = rows // 2
    edge = incl[half - 1 : half]
    top = iota((rows, width), 0) < half
    ref = jnp.where(top, incl[half // 2 - 1 : half // 2], incl[half + half // 2 - 1 : half + half // 2])
    r = r_ref[...].astype(F32)
    k = k_ref[...].astype(F32)
    v = v_ref[...]
    r_in = (r * jnp.exp(excl - ref)).astype(BF16)
    k_in = (k * jnp.exp(ref - incl)).astype(BF16)
    r_off = (r * jnp.exp(jnp.minimum(excl - edge, 0.0))).astype(BF16)
    k_off = (k * jnp.exp(jnp.minimum(edge - incl, 0.0))).astype(BF16)
    rec_ref[...] = (r * jnp.exp(excl)).astype(BF16)
    k_end = (k * jnp.exp(total - incl)).astype(BF16)
    boost = jnp.concatenate([boost_ref[h : h + 1] for h in range(boost_ref.shape[0])], axis=1)
    now = r * boost * k
    row, col = iota((rows, rows), 0), iota((rows, rows), 1)
    same = (row > col) & ((row < half) == (col < half))
    cross = (row >= half) & (col < half)
    left = iota((rows, 128), 1) < 64
    zero = jnp.zeros((), BF16)
    for p in range(width // 128):
        at = slice(128 * p, 128 * p + 128)
        scores, values, sums = [], [], []
        for mask in (left, ~left):
            inner = dot(r_in[:, at], jnp.where(mask, k_in[:, at], zero), NT)
            outer = dot(r_off[:, at], jnp.where(mask, k_off[:, at], zero), NT)
            scores.append(jnp.where(same, inner, jnp.where(cross, outer, 0.0)).astype(BF16))
            values.append(jnp.where(mask, v[:, at], zero))
            sums.append(jnp.sum(jnp.where(mask, now[:, at], 0.0), axis=1, keepdims=True))
        out = dot(jnp.concatenate(scores, axis=1), jnp.concatenate(values, axis=0), NN)
        own_ref[:, at] = out + jnp.where(left, sums[0], sums[1]) * v[:, at].astype(F32)
        state = dot(v[:, at], k_end[:, at], TN)
        pay_ref[0:64, at] = jnp.where(left[0:64], state[0:64], state[64:128]).astype(BF16)
    last = hi_lo(last_row(own_ref))
    pay_ref[64:72, :] = lines(*hi_lo(total), *last, last_row(rec_ref), last_row(skip_ref), last_row(gate_ref))


def apart(state, at):
    left = iota((64, 128), 1) < 64
    here = state[:, at]
    both = [jnp.where(left, here, 0.0), jnp.where(left, 0.0, here)]
    return jnp.concatenate(both, axis=0).astype(BF16)


def pair_kernel(pair_ref, out_ref):
    a, b = pair_ref[0].astype(F32), pair_ref[1].astype(F32)
    last = b[64:65] + b[65:66]
    state = (a[0:64] * jnp.exp(last) + b[0:64]).astype(BF16)
    recall = jnp.broadcast_to(b[68:69], (8, b.shape[1])).astype(BF16)
    own = [
        dot(recall[:, at], apart(a[0:64], at), NT)[0:1]
        for at in (slice(128 * p, 128 * p + 128) for p in range(b.shape[1] // 128))
    ]
    own = b[66:67] + b[67:68] + jnp.concatenate(own, axis=1)
    start = a[64:65] + a[65:66]
    tail = lines(*hi_lo(start + last), *hi_lo(own), b[68:69] * jnp.exp(start), b[69:70], b[70:71])
    for n in range(out_ref.shape[0]):
        out_ref[n, 0:64] = state
        out_ref[n, 64:72] = tail


def middle_kernel(
    chip_ref, core_ref, all_ref, pair_ref, own_ref, rec_ref, skip_ref, gate_ref, gn_ref, ln_ref,
    mid_ref, main_ref, side_ref,
):
    rows, width = own_ref.shape
    main = main_ref.shape[0]

    def join(ref):
        def step(i, state):
            piece = ref[i].astype(F32)
            return state * jnp.exp(piece[64:65] + piece[65:66]) + piece[0:64]

        return step

    chip, core = chip_ref[0], core_ref[0]
    split = jnp.maximum(chip + core - 1, 0)
    old = lax.fori_loop(0, split, join(all_ref), jnp.zeros((64, width), F32))
    state = lax.fori_loop(split, chip, join(all_ref), old)
    state = lax.fori_loop(0, core, join(pair_ref), state)

    def finish(own, recall, skip, gate, before, at):
        left = iota(own.shape, 1) < 64

        def mean(x):
            a = jnp.sum(jnp.where(left, x, 0.0), axis=1, keepdims=True)
            b = jnp.sum(jnp.where(left, 0.0, x), axis=1, keepdims=True)
            return jnp.where(left, a, b) * (1.0 / 64)

        wkv = own + dot(recall, apart(before, at), NT)
        centre = wkv - mean(wkv)
        normed = centre * lax.rsqrt(mean(centre * centre) + EPS_GROUP)
        normed = normed * gn_ref[0:1, at] + gn_ref[1:2, at]
        return skip + normed * (gate / (1.0 + jnp.exp(-gate)))

    line = iota((8, 128), 0)
    prior = all_ref[jnp.maximum(chip - 1, 0)].astype(F32)[64:72]
    prior = jnp.where(core > 0, pair_ref[0].astype(F32)[64:72], prior)
    prior = [prior[2:3] + prior[3:4], prior[4:5], prior[5:6], prior[6:7]]
    for p in range(width // 128):
        at = slice(128 * p, 128 * p + 128)
        middle = finish(
            own_ref[:, at], rec_ref[:, at], skip_ref[:, at].astype(F32), gate_ref[:, at].astype(F32), state, at
        )
        mid_ref[:, at] = middle
        main_ref[:, at] = middle[0:main].astype(BF16)
        own, recall, skip, gate = (jnp.broadcast_to(row[:, at], (8, 128)) for row in prior)
        tail = jnp.where(line == 0, finish(own, recall.astype(BF16), skip, gate, old, at), 0.0)
        for n in range(3):
            hi, lo = hi_lo(ln_ref[n : n + 1, at])
            tail = jnp.where(line == 2 * n + 1, hi.astype(F32), tail)
            tail = jnp.where(line == 2 * n + 2, lo.astype(F32), tail)
        edge, tail = middle[main:].astype(BF16), tail.astype(BF16)
        for g in range(side_ref.shape[0]):
            side_ref[g, 0, :, at] = edge
            side_ref[g, 1, :, at] = tail


def ffn_kernel(seq_ref, zh_ref, main_ref, side_ref, w_hbm, give_ref, hidden_ref, w_ref, sems):
    _, rows, width = give_ref.shape
    groups, main = main_ref.shape[0:2]
    full = groups * width
    depth = w_hbm.shape[1]
    tall = w_hbm.shape[0] // (full // depth)
    units = tall // 2
    chunks = sems.shape[0]
    step = full // chunks

    def copy(q):
        at = pl.ds(q * step // depth * tall, step // depth * tall)
        return pltpu.make_async_copy(w_hbm.at[at], w_ref.at[at], sems.at[q])

    def weights(g, first):
        starts = [(g * (width // depth) + b) * tall + first for b in range(width // depth)]
        if not isinstance(g, int):
            starts = [pl.multiple_of(start, 64) for start in starts]
        return jnp.concatenate([w_ref[pl.ds(start, units)] for start in starts], axis=1)

    for q in range(chunks):
        copy(q).start()

    def load(g):
        return jnp.concatenate([main_ref[g].astype(F32), side_ref[g, 0].astype(F32)], axis=0)

    def stats(get, n):
        first, second = jnp.zeros((n, width), F32), jnp.zeros((n, width), F32)
        for g in range(groups):
            x = get(g)
            first, second = first + x, second + x * x
        mu = jnp.sum(first, axis=1, keepdims=True) / full
        var = jnp.sum(second, axis=1, keepdims=True) / full - mu * mu
        return mu, lax.rsqrt(var + EPS_LAYER)

    mu, scale = stats(load, rows)
    pmu, pscale = stats(lambda g: side_ref[g, 1].astype(F32)[0:1], 1)
    live = seq_ref[0] > 0
    head = iota((rows, width), 0) == 0
    acc = jnp.zeros((rows, units), F32)
    for g in range(groups):
        side = side_ref[g, 1].astype(F32)
        gain, bias, blend = (side[n : n + 1] + side[n + 1 : n + 2] for n in (1, 3, 5))
        xn = ((load(g) - mu) * scale * gain + bias).astype(BF16).astype(F32)
        pn = ((side[0:1] - pmu) * pscale * gain + bias).astype(BF16).astype(F32)
        pn = jnp.where(live, pn, 0.0)
        prev = jnp.where(head, pn, pltpu.roll(xn, 1, 0))
        xk = (xn + (prev - xn) * blend).astype(BF16)
        if g * width % step == 0:
            copy(g * width // step).wait()
        acc = acc + dot(xk, weights(g, 0), NT)
    hidden = jnp.square(jnp.maximum(acc, 0.0)).astype(BF16)
    hidden_ref[...] = hidden
    for g in range(groups // 2):
        give_ref[g] = dot(hidden, weights(2 * g + 1 - zh_ref[0], units), NN).astype(BF16)


def keep_kernel(zh_ref, hidden_ref, w_hbm, keep_ref, w_ref, sems):
    groups, rows, width = keep_ref.shape
    units = hidden_ref.shape[1]
    depth = w_hbm.shape[1]
    each = width // depth

    def copy(g, b):
        start = (((2 * g + zh_ref[0]) * each + b) * 2 + 1) * units
        return pltpu.make_async_copy(
            w_hbm.at[pl.ds(pl.multiple_of(start, 64), units)], w_ref.at[g * each + b], sems.at[g * each + b]
        )

    for g in range(groups):
        for b in range(each):
            copy(g, b).start()
    for g in range(groups):
        for b in range(each):
            copy(g, b).wait()
        w = jnp.concatenate([w_ref[g * each + b] for b in range(each)], axis=1)
        keep_ref[g] = dot(hidden_ref[...], w, NN).astype(BF16)


VMEM = functools.partial(pl.BlockSpec, memory_space=pltpu.VMEM)
SMEM = functools.partial(pl.BlockSpec, memory_space=pltpu.SMEM)


def make(interpret):
    def call(kernel, outs, *args, in_specs=None, **more):
        return pl.pallas_call(
            kernel,
            out_shape=[jax.ShapeDtypeStruct(s, t) for s, t in outs],
            in_specs=in_specs or [VMEM() for _ in args],
            out_specs=[VMEM() for _ in outs],
            interpret=interpret,
            **more,
        )(*args)

    def local(
        skip, recept, keys, values, gating, logit, boost, gn_gain, gn_bias, ln_gain, ln_bias, blend, wk, wv
    ):
        rows, width = skip.shape
        groups = lax.axis_size(HID)
        blocks = lax.axis_size(SEQ)
        at_seq = lax.axis_index(SEQ).reshape(1)

        chips = blocks // lax.axis_size("c")
        chip = lax.axis_index(("y", "x")).reshape(1)
        core = lax.axis_index("c").reshape(1)
        zh = lax.axis_index("zh").reshape(1)
        own, recall, state, weights = call(
            wkv_kernel,
            [
                ((rows, width), F32),
                ((rows, width), BF16),
                ((72, width), BF16),
                ((2 * wk.shape[1], wk.shape[0]), BF16),
            ],
            recept, keys, values, logit, boost, skip, gating, wk.T, wv.T,
        )
        weights = lax.all_gather(weights, SEQ, tiled=True)
        pair = lax.all_gather(state, "c")
        (states,) = call(pair_kernel, [((chips, 72, width), BF16)], pair)
        states = lax.all_to_all(states, ("y", "x"), 0, 0, tiled=True)
        middle, main, side = call(
            middle_kernel,
            [((rows, width), F32), ((rows - 8, width), BF16), ((groups, 2, 8, width), BF16)],
            chip, core, states, pair, own, recall, skip, gating,
            jnp.stack([gn_gain, gn_bias]), jnp.stack([ln_gain, ln_bias, blend]),
            in_specs=[SMEM(), SMEM()] + [VMEM()] * 8,
        )
        side = lax.all_to_all(side, HID, 0, 0, tiled=True)
        main = lax.all_gather(main, HID)
        any_space = pl.BlockSpec(memory_space=pl.ANY)
        units, depth = wk.shape[1], wk.shape[0]
        give, hidden = call(
            ffn_kernel,
            [((groups // 2, rows, width), BF16), ((rows, units), BF16)],
            at_seq, zh, main, side, weights,
            in_specs=[SMEM(), SMEM(), VMEM(), VMEM(), any_space],
            scratch_shapes=[pltpu.VMEM(weights.shape, BF16), pltpu.SemaphoreType.DMA((min(8, groups),))],
        )
        give = lax.ppermute(give, "zh", [(0, 1), (1, 0)])
        (keep,) = call(
            keep_kernel,
            [((groups // 2, rows, width), BF16)],
            zh, hidden, weights,
            in_specs=[SMEM(), VMEM(), any_space],
            scratch_shapes=[pltpu.VMEM((blocks // 2, units, depth), BF16), pltpu.SemaphoreType.DMA((blocks // 2,))],
        )
        part = (keep.astype(F32) + give.astype(F32)).astype(BF16)
        part = lax.all_to_all(part, "zl", 0, 0, tiled=True)
        return (middle + jnp.sum(part.astype(F32), axis=0)).astype(BF16)

    return local


def build(finer, interpret=False):
    tile, vec = P(SEQ, HID), P(HID)
    return jax.shard_map(
        make(interpret),
        mesh=finer,
        in_specs=(tile,) * 6 + (P(HID, None),) + (vec,) * 5 + (tile, tile),
        out_specs=tile,
        check_vma=False,
    )


def solution(mesh):
    return build(Mesh(mesh.devices.reshape(4, 4, 2, mesh.shape["hid"] // 2, 2), (*SEQ, *HID)))
```

```python
import functools

import jax
import jax.numpy as jnp
from jax import lax
from jax.experimental import pallas as pl
from jax.experimental.pallas import tpu as pltpu
from jax.sharding import Mesh
from jax.sharding import PartitionSpec as P

SEQ = ("y", "x", "c")
HID = ("zl", "zh")
EPS_GROUP = 0.00064
EPS_LAYER = 1e-05
F32 = jnp.float32
BF16 = jnp.bfloat16
NN = (((1,), (0,)), ((), ()))
NT = (((1,), (1,)), ((), ()))
TN = (((0,), (0,)), ((), ()))


def dot(a, b, dims):
    return lax.dot_general(a, b, dims, preferred_element_type=F32)


def iota(shape, dim):
    return lax.broadcasted_iota(jnp.int32, shape, dim)


def hi_lo(x):
    hi = x.astype(BF16)
    return hi, (x - hi.astype(F32)).astype(BF16)


def last_row(ref):
    rows = ref.shape[0]
    return ref[rows - 16 : rows, :].astype(F32)[15:16]


def lines(*rows):
    width = rows[0].shape[1]
    line = iota((8, width), 0)
    tile = jnp.zeros((8, width), F32)
    for n, row in enumerate(rows):
        tile = jnp.where(line == n, row.astype(F32), tile)
    return tile.astype(BF16)


def wkv_kernel(
    r_ref, k_ref, v_ref, logit_ref, boost_ref, skip_ref, gate_ref, wk_ref, wv_ref,
    own_ref, rec_ref, pay_ref, w_ref,
):
    units = wk_ref.shape[0]
    w_ref[0:units] = wk_ref[...]
    w_ref[units:] = wv_ref[...]
    rows, width = r_ref.shape
    logw = -jnp.exp(logit_ref[...])
    lower = (iota((rows, rows), 0) >= iota((rows, rows), 1)).astype(BF16)
    part0, rest = logw.astype(BF16), logw
    rest = rest - part0.astype(F32)
    part1, part2 = hi_lo(rest)
    incl = dot(lower, part0, NN) + dot(lower, part1, NN) + dot(lower, part2, NN)
    excl = incl - logw
    total = incl[rows - 1 : rows]
    half = rows // 2
    edge = incl[half - 1 : half]
    top = iota((rows, width), 0) < half
    ref = jnp.where(top, incl[half // 2 - 1 : half // 2], incl[half + half // 2 - 1 : half + half // 2])
    r = r_ref[...].astype(F32)
    k = k_ref[...].astype(F32)
    v = v_ref[...]
    r_in = (r * jnp.exp(excl - ref)).astype(BF16)
    k_in = (k * jnp.exp(ref - incl)).astype(BF16)
    r_off = (r * jnp.exp(jnp.minimum(excl - edge, 0.0))).astype(BF16)
    k_off = (k * jnp.exp(jnp.minimum(edge - incl, 0.0))).astype(BF16)
    rec_ref[...] = (r * jnp.exp(excl)).astype(BF16)
    k_end = (k * jnp.exp(total - incl)).astype(BF16)
    boost = jnp.concatenate([boost_ref[h : h + 1] for h in range(boost_ref.shape[0])], axis=1)
    now = r * boost * k
    row, col = iota((rows, rows), 0), iota((rows, rows), 1)
    same = (row > col) & ((row < half) == (col < half))
    cross = (row >= half) & (col < half)
    left = iota((rows, 128), 1) < 64
    zero = jnp.zeros((), BF16)
    for p in range(width // 128):
        at = slice(128 * p, 128 * p + 128)
        scores, values, sums = [], [], []
        for mask in (left, ~left):
            inner = dot(r_in[:, at], jnp.where(mask, k_in[:, at], zero), NT)
            outer = dot(r_off[:, at], jnp.where(mask, k_off[:, at], zero), NT)
            scores.append(jnp.where(same, inner, jnp.where(cross, outer, 0.0)).astype(BF16))
            values.append(jnp.where(mask, v[:, at], zero))
            sums.append(jnp.sum(jnp.where(mask, now[:, at], 0.0), axis=1, keepdims=True))
        out = dot(jnp.concatenate(scores, axis=1), jnp.concatenate(values, axis=0), NN)
        own_ref[:, at] = out + jnp.where(left, sums[0], sums[1]) * v[:, at].astype(F32)
        state = dot(v[:, at], k_end[:, at], TN)
        pay_ref[0:64, at] = jnp.where(left[0:64], state[0:64], state[64:128]).astype(BF16)
    last = hi_lo(last_row(own_ref))
    pay_ref[64:72, :] = lines(*hi_lo(total), *last, last_row(rec_ref), last_row(skip_ref), last_row(gate_ref))


def apart(state, at):
    left = iota((64, 128), 1) < 64
    here = state[:, at]
    both = [jnp.where(left, here, 0.0), jnp.where(left, 0.0, here)]
    return jnp.concatenate(both, axis=0).astype(BF16)


def pair_kernel(pair_ref, out_ref):
    a, b = pair_ref[0].astype(F32), pair_ref[1].astype(F32)
    last = b[64:65] + b[65:66]
    state = (a[0:64] * jnp.exp(last) + b[0:64]).astype(BF16)
    recall = jnp.broadcast_to(b[68:69], (8, b.shape[1])).astype(BF16)
    own = [
        dot(recall[:, at], apart(a[0:64], at), NT)[0:1]
        for at in (slice(128 * p, 128 * p + 128) for p in range(b.shape[1] // 128))
    ]
    own = b[66:67] + b[67:68] + jnp.concatenate(own, axis=1)
    start = a[64:65] + a[65:66]
    tail = lines(*hi_lo(start + last), *hi_lo(own), b[68:69] * jnp.exp(start), b[69:70], b[70:71])
    for n in range(out_ref.shape[0]):
        out_ref[n, 0:64] = state
        out_ref[n, 64:72] = tail


def middle_kernel(
    chip_ref, core_ref, all_ref, pair_ref, own_ref, rec_ref, skip_ref, gate_ref, gn_ref, ln_ref,
    mid_ref, send_ref,
):
    rows, width = own_ref.shape

    def join(ref):
        def step(i, state):
            piece = ref[i].astype(F32)
            return state * jnp.exp(piece[64:65] + piece[65:66]) + piece[0:64]

        return step

    chip, core = chip_ref[0], core_ref[0]
    split = jnp.maximum(chip + core - 1, 0)
    old = lax.fori_loop(0, split, join(all_ref), jnp.zeros((64, width), F32))
    state = lax.fori_loop(split, chip, join(all_ref), old)
    state = lax.fori_loop(0, core, join(pair_ref), state)

    def finish(own, recall, skip, gate, before, at):
        left = iota(own.shape, 1) < 64

        def mean(x):
            a = jnp.sum(jnp.where(left, x, 0.0), axis=1, keepdims=True)
            b = jnp.sum(jnp.where(left, 0.0, x), axis=1, keepdims=True)
            return jnp.where(left, a, b) * (1.0 / 64)

        wkv = own + dot(recall, apart(before, at), NT)
        centre = wkv - mean(wkv)
        normed = centre * lax.rsqrt(mean(centre * centre) + EPS_GROUP)
        normed = normed * gn_ref[0:1, at] + gn_ref[1:2, at]
        return skip + normed * (gate / (1.0 + jnp.exp(-gate)))

    line = iota((8, 128), 0)
    prior = all_ref[jnp.maximum(chip - 1, 0)].astype(F32)[64:72]
    prior = jnp.where(core > 0, pair_ref[0].astype(F32)[64:72], prior)
    prior = [prior[2:3] + prior[3:4], prior[4:5], prior[5:6], prior[6:7]]
    for p in range(width // 128):
        at = slice(128 * p, 128 * p + 128)
        middle = finish(
            own_ref[:, at], rec_ref[:, at], skip_ref[:, at].astype(F32), gate_ref[:, at].astype(F32), state, at
        )
        mid_ref[:, at] = middle
        own, recall, skip, gate = (jnp.broadcast_to(row[:, at], (8, 128)) for row in prior)
        tail = jnp.where(line == 0, finish(own, recall.astype(BF16), skip, gate, old, at), 0.0)
        for n in range(3):
            hi, lo = hi_lo(ln_ref[n : n + 1, at])
            tail = jnp.where(line == 2 * n + 1, hi.astype(F32), tail)
            tail = jnp.where(line == 2 * n + 2, lo.astype(F32), tail)
        middle, tail = middle.astype(BF16), tail.astype(BF16)
        for g in range(send_ref.shape[0]):
            send_ref[g, 0:rows, at] = middle
            send_ref[g, rows:, at] = tail


def ffn_kernel(seq_ref, zh_ref, even_ref, odd_ref, w_hbm, give_ref, hidden_ref, w_ref, sems):
    half, rows, width = give_ref.shape
    groups = 2 * half
    full = groups * width
    depth = w_hbm.shape[1]
    tall = w_hbm.shape[0] // (full // depth)
    units = tall // 2
    chunks = sems.shape[0]
    step = full // chunks

    def copy(q):
        at = pl.ds(q * step // depth * tall, step // depth * tall)
        return pltpu.make_async_copy(w_hbm.at[at], w_ref.at[at], sems.at[q])

    def weights(g, first):
        starts = [(g * (width // depth) + b) * tall + first for b in range(width // depth)]
        if not isinstance(g, int):
            starts = [pl.multiple_of(start, 64) for start in starts]
        return jnp.concatenate([w_ref[pl.ds(start, units)] for start in starts], axis=1)

    for q in range(chunks):
        copy(q).start()

    parts = [(ref, j, 2 * j + place) for j in range(half) for ref, place in ((even_ref, zh_ref[0]), (odd_ref, 1 - zh_ref[0]))]

    def stats(first_row, last_row, n):
        first, second = jnp.zeros((n, width), F32), jnp.zeros((n, width), F32)
        for ref, j, _ in parts:
            x = ref[j, first_row:last_row].astype(F32)[0:n]
            first, second = first + x, second + x * x
        mu = jnp.sum(first, axis=1, keepdims=True) / full
        var = jnp.sum(second, axis=1, keepdims=True) / full - mu * mu
        return mu, lax.rsqrt(var + EPS_LAYER)

    mu, scale = stats(0, rows, rows)
    pmu, pscale = stats(rows, rows + 8, 1)
    live = seq_ref[0] > 0
    head = iota((rows, width), 0) == 0
    acc = jnp.zeros((rows, units), F32)
    waited = 0
    for ref, j, g in parts:
        side = ref[j, rows : rows + 8].astype(F32)
        gain, bias, blend = (side[n : n + 1] + side[n + 1 : n + 2] for n in (1, 3, 5))
        xn = ((ref[j, 0:rows].astype(F32) - mu) * scale * gain + bias).astype(BF16).astype(F32)
        pn = ((side[0:1] - pmu) * pscale * gain + bias).astype(BF16).astype(F32)
        pn = jnp.where(live, pn, 0.0)
        prev = jnp.where(head, pn, pltpu.roll(xn, 1, 0))
        xk = (xn + (prev - xn) * blend).astype(BF16)
        while waited * step < 2 * (j + 1) * width:
            copy(waited).wait()
            waited += 1
        acc = acc + dot(xk, weights(g, 0), NT)
    hidden = jnp.square(jnp.maximum(acc, 0.0)).astype(BF16)
    hidden_ref[...] = hidden
    for g in range(groups // 2):
        give_ref[g] = dot(hidden, weights(2 * g + 1 - zh_ref[0], units), NN).astype(BF16)


def keep_kernel(zh_ref, hidden_ref, w_hbm, keep_ref, w_ref, sems):
    groups, rows, width = keep_ref.shape
    units = hidden_ref.shape[1]
    depth = w_hbm.shape[1]
    each = width // depth

    def copy(g, b):
        start = (((2 * g + zh_ref[0]) * each + b) * 2 + 1) * units
        return pltpu.make_async_copy(
            w_hbm.at[pl.ds(pl.multiple_of(start, 64), units)], w_ref.at[g * each + b], sems.at[g * each + b]
        )

    for g in range(groups):
        for b in range(each):
            copy(g, b).start()
    for g in range(groups):
        for b in range(each):
            copy(g, b).wait()
        w = jnp.concatenate([w_ref[g * each + b] for b in range(each)], axis=1)
        keep_ref[g] = dot(hidden_ref[...], w, NN).astype(BF16)


VMEM = functools.partial(pl.BlockSpec, memory_space=pltpu.VMEM)
SMEM = functools.partial(pl.BlockSpec, memory_space=pltpu.SMEM)


def make(interpret):
    def call(kernel, outs, *args, in_specs=None, **more):
        return pl.pallas_call(
            kernel,
            out_shape=[jax.ShapeDtypeStruct(s, t) for s, t in outs],
            in_specs=in_specs or [VMEM() for _ in args],
            out_specs=[VMEM() for _ in outs],
            interpret=interpret,
            **more,
        )(*args)

    def local(
        skip, recept, keys, values, gating, logit, boost, gn_gain, gn_bias, ln_gain, ln_bias, blend, wk, wv
    ):
        rows, width = skip.shape
        groups = lax.axis_size(HID)
        blocks = lax.axis_size(SEQ)
        at_seq = lax.axis_index(SEQ).reshape(1)

        chips = blocks // lax.axis_size("c")
        chip = lax.axis_index(("y", "x")).reshape(1)
        core = lax.axis_index("c").reshape(1)
        zh = lax.axis_index("zh").reshape(1)
        own, recall, state, weights = call(
            wkv_kernel,
            [
                ((rows, width), F32),
                ((rows, width), BF16),
                ((72, width), BF16),
                ((2 * wk.shape[1], wk.shape[0]), BF16),
            ],
            recept, keys, values, logit, boost, skip, gating, wk.T, wv.T,
        )
        weights = lax.all_gather(weights, SEQ, tiled=True)
        pair = lax.all_gather(state, "c")
        (states,) = call(pair_kernel, [((chips, 72, width), BF16)], pair)
        states = lax.all_to_all(states, ("y", "x"), 0, 0, tiled=True)
        middle, send = call(
            middle_kernel,
            [((rows, width), F32), ((groups // 2, rows + 8, width), BF16)],
            chip, core, states, pair, own, recall, skip, gating,
            jnp.stack([gn_gain, gn_bias]), jnp.stack([ln_gain, ln_bias, blend]),
            in_specs=[SMEM(), SMEM()] + [VMEM()] * 8,
        )
        mine = lax.all_to_all(send, "zl", 0, 0, tiled=True)
        other = lax.ppermute(mine, "zh", [(0, 1), (1, 0)])
        any_space = pl.BlockSpec(memory_space=pl.ANY)
        units, depth = wk.shape[1], wk.shape[0]
        give, hidden = call(
            ffn_kernel,
            [((groups // 2, rows, width), BF16), ((rows, units), BF16)],
            at_seq, zh, mine, other, weights,
            in_specs=[SMEM(), SMEM(), VMEM(), VMEM(), any_space],
            scratch_shapes=[pltpu.VMEM(weights.shape, BF16), pltpu.SemaphoreType.DMA((min(8, groups),))],
        )
        give = lax.ppermute(give, "zh", [(0, 1), (1, 0)])
        (keep,) = call(
            keep_kernel,
            [((groups // 2, rows, width), BF16)],
            zh, hidden, weights,
            in_specs=[SMEM(), VMEM(), any_space],
            scratch_shapes=[pltpu.VMEM((blocks // 2, units, depth), BF16), pltpu.SemaphoreType.DMA((blocks // 2,))],
        )
        part = (keep.astype(F32) + give.astype(F32)).astype(BF16)
        part = lax.all_to_all(part, "zl", 0, 0, tiled=True)
        return (middle + jnp.sum(part.astype(F32), axis=0)).astype(BF16)

    return local


def build(finer, interpret=False):
    tile, vec = P(SEQ, HID), P(HID)
    return jax.shard_map(
        make(interpret),
        mesh=finer,
        in_specs=(tile,) * 6 + (P(HID, None),) + (vec,) * 5 + (tile, tile),
        out_specs=tile,
        check_vma=False,
    )


def solution(mesh):
    return build(Mesh(mesh.devices.reshape(4, 4, 2, mesh.shape["hid"] // 2, 2), (*SEQ, *HID)))
```

```python
import functools

import jax
import jax.numpy as jnp
from jax import lax
from jax.experimental import pallas as pl
from jax.experimental.pallas import tpu as pltpu
from jax.sharding import Mesh
from jax.sharding import PartitionSpec as P

SEQ = ("y", "x", "c")
HID = ("zl", "zh")
EPS_GROUP = 0.00064
EPS_LAYER = 1e-05
F32 = jnp.float32
BF16 = jnp.bfloat16
NN = (((1,), (0,)), ((), ()))
NT = (((1,), (1,)), ((), ()))
TN = (((0,), (0,)), ((), ()))


def dot(a, b, dims):
    return lax.dot_general(a, b, dims, preferred_element_type=F32)


def iota(shape, dim):
    return lax.broadcasted_iota(jnp.int32, shape, dim)


def hi_lo(x):
    hi = x.astype(BF16)
    return hi, (x - hi.astype(F32)).astype(BF16)


def last_row(ref):
    rows = ref.shape[0]
    return ref[rows - 16 : rows, :].astype(F32)[15:16]


def lines(*rows):
    width = rows[0].shape[1]
    line = iota((8, width), 0)
    tile = jnp.zeros((8, width), F32)
    for n, row in enumerate(rows):
        tile = jnp.where(line == n, row.astype(F32), tile)
    return tile.astype(BF16)


def wkv_kernel(
    r_ref, k_ref, v_ref, logit_ref, boost_ref, skip_ref, gate_ref, wk_ref, wv_ref,
    own_ref, rec_ref, pay_ref, w_ref,
):
    units = wk_ref.shape[0]
    w_ref[0:units] = wk_ref[...]
    w_ref[units:] = wv_ref[...]
    rows, width = r_ref.shape
    logw = -jnp.exp(logit_ref[...])
    lower = (iota((rows, rows), 0) >= iota((rows, rows), 1)).astype(BF16)
    part0, rest = logw.astype(BF16), logw
    rest = rest - part0.astype(F32)
    part1, part2 = hi_lo(rest)
    incl = dot(lower, part0, NN) + dot(lower, part1, NN) + dot(lower, part2, NN)
    excl = incl - logw
    total = incl[rows - 1 : rows]
    half = rows // 2
    edge = incl[half - 1 : half]
    top = iota((rows, width), 0) < half
    ref = jnp.where(top, incl[half // 2 - 1 : half // 2], incl[half + half // 2 - 1 : half + half // 2])
    r = r_ref[...].astype(F32)
    k = k_ref[...].astype(F32)
    v = v_ref[...]
    r_in = (r * jnp.exp(excl - ref)).astype(BF16)
    k_in = (k * jnp.exp(ref - incl)).astype(BF16)
    r_off = (r * jnp.exp(jnp.minimum(excl - edge, 0.0))).astype(BF16)
    k_off = (k * jnp.exp(jnp.minimum(edge - incl, 0.0))).astype(BF16)
    rec_ref[...] = (r * jnp.exp(excl)).astype(BF16)
    k_end = (k * jnp.exp(total - incl)).astype(BF16)
    boost = jnp.concatenate([boost_ref[h : h + 1] for h in range(boost_ref.shape[0])], axis=1)
    now = r * boost * k
    row, col = iota((rows, rows), 0), iota((rows, rows), 1)
    same = (row > col) & ((row < half) == (col < half))
    cross = (row >= half) & (col < half)
    left = iota((rows, 128), 1) < 64
    zero = jnp.zeros((), BF16)
    for p in range(width // 128):
        at = slice(128 * p, 128 * p + 128)
        scores, values, sums = [], [], []
        for mask in (left, ~left):
            inner = dot(r_in[:, at], jnp.where(mask, k_in[:, at], zero), NT)
            outer = dot(r_off[:, at], jnp.where(mask, k_off[:, at], zero), NT)
            scores.append(jnp.where(same, inner, jnp.where(cross, outer, 0.0)).astype(BF16))
            values.append(jnp.where(mask, v[:, at], zero))
            sums.append(jnp.sum(jnp.where(mask, now[:, at], 0.0), axis=1, keepdims=True))
        out = dot(jnp.concatenate(scores, axis=1), jnp.concatenate(values, axis=0), NN)
        own_ref[:, at] = out + jnp.where(left, sums[0], sums[1]) * v[:, at].astype(F32)
        state = dot(v[:, at], k_end[:, at], TN)
        pay_ref[0:64, at] = jnp.where(left[0:64], state[0:64], state[64:128]).astype(BF16)
    last = hi_lo(last_row(own_ref))
    pay_ref[64:72, :] = lines(*hi_lo(total), *last, last_row(rec_ref), last_row(skip_ref), last_row(gate_ref))


def apart(state, at):
    left = iota((64, 128), 1) < 64
    here = state[:, at]
    both = [jnp.where(left, here, 0.0), jnp.where(left, 0.0, here)]
    return jnp.concatenate(both, axis=0).astype(BF16)


def pair_kernel(pair_ref, out_ref):
    a, b = pair_ref[0].astype(F32), pair_ref[1].astype(F32)
    last = b[64:65] + b[65:66]
    state = (a[0:64] * jnp.exp(last) + b[0:64]).astype(BF16)
    recall = jnp.broadcast_to(b[68:69], (8, b.shape[1])).astype(BF16)
    own = [
        dot(recall[:, at], apart(a[0:64], at), NT)[0:1]
        for at in (slice(128 * p, 128 * p + 128) for p in range(b.shape[1] // 128))
    ]
    own = b[66:67] + b[67:68] + jnp.concatenate(own, axis=1)
    start = a[64:65] + a[65:66]
    tail = lines(*hi_lo(start + last), *hi_lo(own), b[68:69] * jnp.exp(start), b[69:70], b[70:71])
    for n in range(out_ref.shape[0]):
        out_ref[n, 0:64] = state
        out_ref[n, 64:72] = tail


def middle_kernel(
    chip_ref, core_ref, all_ref, pair_ref, own_ref, rec_ref, skip_ref, gate_ref, gn_ref, ln_ref,
    mid_ref, main_ref, side_ref,
):
    rows, width = own_ref.shape
    main = main_ref.shape[0]

    def join(ref):
        def step(i, state):
            piece = ref[i].astype(F32)
            return state * jnp.exp(piece[64:65] + piece[65:66]) + piece[0:64]

        return step

    chip, core = chip_ref[0], core_ref[0]
    split = jnp.maximum(chip + core - 1, 0)
    old = lax.fori_loop(0, split, join(all_ref), jnp.zeros((64, width), F32))
    state = lax.fori_loop(split, chip, join(all_ref), old)
    state = lax.fori_loop(0, core, join(pair_ref), state)

    def finish(own, recall, skip, gate, before, at):
        left = iota(own.shape, 1) < 64

        def mean(x):
            a = jnp.sum(jnp.where(left, x, 0.0), axis=1, keepdims=True)
            b = jnp.sum(jnp.where(left, 0.0, x), axis=1, keepdims=True)
            return jnp.where(left, a, b) * (1.0 / 64)

        wkv = own + dot(recall, apart(before, at), NT)
        centre = wkv - mean(wkv)
        normed = centre * lax.rsqrt(mean(centre * centre) + EPS_GROUP)
        normed = normed * gn_ref[0:1, at] + gn_ref[1:2, at]
        return skip + normed * (gate / (1.0 + jnp.exp(-gate)))

    line = iota((8, 128), 0)
    prior = all_ref[jnp.maximum(chip - 1, 0)].astype(F32)[64:72]
    prior = jnp.where(core > 0, pair_ref[0].astype(F32)[64:72], prior)
    prior = [prior[2:3] + prior[3:4], prior[4:5], prior[5:6], prior[6:7]]
    for p in range(width // 128):
        at = slice(128 * p, 128 * p + 128)
        middle = finish(
            own_ref[:, at], rec_ref[:, at], skip_ref[:, at].astype(F32), gate_ref[:, at].astype(F32), state, at
        )
        mid_ref[:, at] = middle
        main_ref[:, at] = middle[0:main].astype(BF16)
        own, recall, skip, gate = (jnp.broadcast_to(row[:, at], (8, 128)) for row in prior)
        tail = jnp.where(line == 0, finish(own, recall.astype(BF16), skip, gate, old, at), 0.0)
        for n in range(3):
            hi, lo = hi_lo(ln_ref[n : n + 1, at])
            tail = jnp.where(line == 2 * n + 1, hi.astype(F32), tail)
            tail = jnp.where(line == 2 * n + 2, lo.astype(F32), tail)
        edge, tail = middle[main:].astype(BF16), tail.astype(BF16)
        for g in range(side_ref.shape[0]):
            side_ref[g, 0, :, at] = edge
            side_ref[g, 1, :, at] = tail


def ffn_kernel(seq_ref, zh_ref, main_ref, side_ref, w_hbm, give_ref, hidden_ref, w_ref, sems):
    _, rows, width = give_ref.shape
    groups, main = main_ref.shape[0:2]
    full = groups * width
    depth = w_hbm.shape[1]
    tall = w_hbm.shape[0] // (full // depth)
    units = tall // 2
    chunks = sems.shape[0]
    step = full // chunks

    def copy(q):
        at = pl.ds(q * step // depth * tall, step // depth * tall)
        return pltpu.make_async_copy(w_hbm.at[at], w_ref.at[at], sems.at[q])

    def weights(g, first):
        starts = [(g * (width // depth) + b) * tall + first for b in range(width // depth)]
        if not isinstance(g, int):
            starts = [pl.multiple_of(start, 64) for start in starts]
        return jnp.concatenate([w_ref[pl.ds(start, units)] for start in starts], axis=1)

    for q in range(chunks):
        copy(q).start()

    def load(g):
        return jnp.concatenate([main_ref[g].astype(F32), side_ref[g, 0].astype(F32)], axis=0)

    def stats(get, n):
        first, second = jnp.zeros((n, width), F32), jnp.zeros((n, width), F32)
        for g in range(groups):
            x = get(g)
            first, second = first + x, second + x * x
        mu = jnp.sum(first, axis=1, keepdims=True) / full
        var = jnp.sum(second, axis=1, keepdims=True) / full - mu * mu
        return mu, lax.rsqrt(var + EPS_LAYER)

    mu, scale = stats(load, rows)
    pmu, pscale = stats(lambda g: side_ref[g, 1].astype(F32)[0:1], 1)
    live = seq_ref[0] > 0
    head = iota((rows, width), 0) == 0
    acc = jnp.zeros((rows, units), F32)
    for g in range(groups):
        side = side_ref[g, 1].astype(F32)
        gain, bias, blend = (side[n : n + 1] + side[n + 1 : n + 2] for n in (1, 3, 5))
        xn = ((load(g) - mu) * scale * gain + bias).astype(BF16).astype(F32)
        pn = ((side[0:1] - pmu) * pscale * gain + bias).astype(BF16).astype(F32)
        pn = jnp.where(live, pn, 0.0)
        prev = jnp.where(head, pn, pltpu.roll(xn, 1, 0))
        xk = (xn + (prev - xn) * blend).astype(BF16)
        if g * width % step == 0:
            copy(g * width // step).wait()
        acc = acc + dot(xk, weights(g, 0), NT)
    hidden = jnp.square(jnp.maximum(acc, 0.0)).astype(BF16)
    hidden_ref[...] = hidden
    for g in range(groups // 2):
        give_ref[g] = dot(hidden, weights(2 * g + 1 - zh_ref[0], units), NN).astype(BF16)


def keep_kernel(zh_ref, hidden_ref, w_hbm, keep_ref, w_ref, sems):
    groups, rows, width = keep_ref.shape
    units = hidden_ref.shape[1]
    depth = w_hbm.shape[1]
    each = width // depth

    def copy(g, b):
        start = (((2 * g + zh_ref[0]) * each + b) * 2 + 1) * units
        return pltpu.make_async_copy(
            w_hbm.at[pl.ds(pl.multiple_of(start, 64), units)], w_ref.at[g * each + b], sems.at[g * each + b]
        )

    for g in range(groups):
        for b in range(each):
            copy(g, b).start()
    for g in range(groups):
        for b in range(each):
            copy(g, b).wait()
        w = jnp.concatenate([w_ref[g * each + b] for b in range(each)], axis=1)
        keep_ref[g] = dot(hidden_ref[...], w, NN).astype(BF16)


VMEM = functools.partial(pl.BlockSpec, memory_space=pltpu.VMEM)
SMEM = functools.partial(pl.BlockSpec, memory_space=pltpu.SMEM)


def near(x):
    return pltpu.with_memory_space_constraint(x, pltpu.VMEM)


def make(interpret):
    def call(kernel, outs, *args, in_specs=None, **more):
        return pl.pallas_call(
            kernel,
            out_shape=[pltpu.HBM(s, t) if len(s) == 2 and s[0] > 512 else pltpu.VMEM(s, t) for s, t in outs],
            in_specs=in_specs or [VMEM() for _ in args],
            out_specs=[VMEM() for _ in outs],
            interpret=interpret,
            **more,
        )(*args)

    def local(
        skip, recept, keys, values, gating, logit, boost, gn_gain, gn_bias, ln_gain, ln_bias, blend, wk, wv
    ):
        rows, width = skip.shape
        groups = lax.axis_size(HID)
        blocks = lax.axis_size(SEQ)
        at_seq = lax.axis_index(SEQ).reshape(1)

        chips = blocks // lax.axis_size("c")
        chip = lax.axis_index(("y", "x")).reshape(1)
        core = lax.axis_index("c").reshape(1)
        zh = lax.axis_index("zh").reshape(1)
        own, recall, state, weights = call(
            wkv_kernel,
            [
                ((rows, width), F32),
                ((rows, width), BF16),
                ((72, width), BF16),
                ((2 * wk.shape[1], wk.shape[0]), BF16),
            ],
            recept, keys, values, logit, boost, skip, gating, wk.T, wv.T,
        )
        weights = lax.all_gather(weights, SEQ, tiled=True)
        pair = lax.all_gather(state, "c")
        (states,) = call(pair_kernel, [((chips, 72, width), BF16)], near(pair))
        states = lax.all_to_all(states, ("y", "x"), 0, 0, tiled=True)
        middle, main, side = call(
            middle_kernel,
            [((rows, width), F32), ((rows - 8, width), BF16), ((groups, 2, 8, width), BF16)],
            chip, core, near(states), near(pair), near(own), near(recall), skip, gating,
            jnp.stack([gn_gain, gn_bias]), jnp.stack([ln_gain, ln_bias, blend]),
            in_specs=[SMEM(), SMEM()] + [VMEM()] * 8,
        )
        side = lax.all_to_all(side, HID, 0, 0, tiled=True)
        main = lax.all_gather(main, HID)
        any_space = pl.BlockSpec(memory_space=pl.ANY)
        units, depth = wk.shape[1], wk.shape[0]
        give, hidden = call(
            ffn_kernel,
            [((groups // 2, rows, width), BF16), ((rows, units), BF16)],
            at_seq, zh, main, near(side), weights,
            in_specs=[SMEM(), SMEM(), VMEM(), VMEM(), any_space],
            scratch_shapes=[pltpu.VMEM(weights.shape, BF16), pltpu.SemaphoreType.DMA((min(8, groups),))],
        )
        give = lax.ppermute(give, "zh", [(0, 1), (1, 0)])
        (keep,) = call(
            keep_kernel,
            [((groups // 2, rows, width), BF16)],
            zh, near(hidden), weights,
            in_specs=[SMEM(), VMEM(), any_space],
            scratch_shapes=[pltpu.VMEM((blocks // 2, units, depth), BF16), pltpu.SemaphoreType.DMA((blocks // 2,))],
        )
        part = (keep.astype(F32) + give.astype(F32)).astype(BF16)
        part = lax.all_to_all(part, "zl", 0, 0, tiled=True)
        return (middle + jnp.sum(part.astype(F32), axis=0)).astype(BF16)

    return local


def build(finer, interpret=False):
    tile, vec = P(SEQ, HID), P(HID)
    return jax.shard_map(
        make(interpret),
        mesh=finer,
        in_specs=(tile,) * 6 + (P(HID, None),) + (vec,) * 5 + (tile, tile),
        out_specs=tile,
        check_vma=False,
    )


def solution(mesh):
    return build(Mesh(mesh.devices.reshape(4, 4, 2, mesh.shape["hid"] // 2, 2), (*SEQ, *HID)))
```

```python
import functools

import jax
import jax.numpy as jnp
from jax import lax
from jax.experimental import pallas as pl
from jax.experimental.pallas import tpu as pltpu
from jax.sharding import Mesh
from jax.sharding import PartitionSpec as P

SEQ = ("y", "x", "c")
HID = ("zl", "zh")
EPS_GROUP = 0.00064
EPS_LAYER = 1e-05
F32 = jnp.float32
BF16 = jnp.bfloat16
NN = (((1,), (0,)), ((), ()))
NT = (((1,), (1,)), ((), ()))
TN = (((0,), (0,)), ((), ()))


def dot(a, b, dims):
    return lax.dot_general(a, b, dims, preferred_element_type=F32)


def iota(shape, dim):
    return lax.broadcasted_iota(jnp.int32, shape, dim)


def hi_lo(x):
    hi = x.astype(BF16)
    return hi, (x - hi.astype(F32)).astype(BF16)


def last_row(ref):
    rows = ref.shape[0]
    return ref[rows - 16 : rows, :].astype(F32)[15:16]


def lines(*rows):
    width = rows[0].shape[1]
    line = iota((8, width), 0)
    tile = jnp.zeros((8, width), F32)
    for n, row in enumerate(rows):
        tile = jnp.where(line == n, row.astype(F32), tile)
    return tile.astype(BF16)


def wkv_kernel(
    r_ref, k_ref, v_ref, logit_ref, boost_ref, skip_ref, gate_ref, own_ref, rec_ref, pay_ref
):
    rows, width = r_ref.shape
    logw = -jnp.exp(logit_ref[...])
    lower = (iota((rows, rows), 0) >= iota((rows, rows), 1)).astype(BF16)
    part0, rest = logw.astype(BF16), logw
    rest = rest - part0.astype(F32)
    part1, part2 = hi_lo(rest)
    incl = dot(lower, part0, NN) + dot(lower, part1, NN) + dot(lower, part2, NN)
    excl = incl - logw
    total = incl[rows - 1 : rows]
    half = rows // 2
    edge = incl[half - 1 : half]
    top = iota((rows, width), 0) < half
    ref = jnp.where(top, incl[half // 2 - 1 : half // 2], incl[half + half // 2 - 1 : half + half // 2])
    r = r_ref[...].astype(F32)
    k = k_ref[...].astype(F32)
    v = v_ref[...]
    r_in = (r * jnp.exp(excl - ref)).astype(BF16)
    k_in = (k * jnp.exp(ref - incl)).astype(BF16)
    r_off = (r * jnp.exp(jnp.minimum(excl - edge, 0.0))).astype(BF16)
    k_off = (k * jnp.exp(jnp.minimum(edge - incl, 0.0))).astype(BF16)
    rec_ref[...] = (r * jnp.exp(excl)).astype(BF16)
    k_end = (k * jnp.exp(total - incl)).astype(BF16)
    boost = jnp.concatenate([boost_ref[h : h + 1] for h in range(boost_ref.shape[0])], axis=1)
    now = r * boost * k
    row, col = iota((rows, rows), 0), iota((rows, rows), 1)
    same = (row > col) & ((row < half) == (col < half))
    cross = (row >= half) & (col < half)
    left = iota((rows, 128), 1) < 64
    zero = jnp.zeros((), BF16)
    for p in range(width // 128):
        at = slice(128 * p, 128 * p + 128)
        scores, values, sums = [], [], []
        for mask in (left, ~left):
            inner = dot(r_in[:, at], jnp.where(mask, k_in[:, at], zero), NT)
            outer = dot(r_off[:, at], jnp.where(mask, k_off[:, at], zero), NT)
            scores.append(jnp.where(same, inner, jnp.where(cross, outer, 0.0)).astype(BF16))
            values.append(jnp.where(mask, v[:, at], zero))
            sums.append(jnp.sum(jnp.where(mask, now[:, at], 0.0), axis=1, keepdims=True))
        out = dot(jnp.concatenate(scores, axis=1), jnp.concatenate(values, axis=0), NN)
        own_ref[:, at] = out + jnp.where(left, sums[0], sums[1]) * v[:, at].astype(F32)
        state = dot(v[:, at], k_end[:, at], TN)
        pay_ref[0:64, at] = jnp.where(left[0:64], state[0:64], state[64:128]).astype(BF16)
    last = hi_lo(last_row(own_ref))
    pay_ref[64:72, :] = lines(*hi_lo(total), *last, last_row(rec_ref), last_row(skip_ref), last_row(gate_ref))


def apart(state, at):
    left = iota((64, 128), 1) < 64
    here = state[:, at]
    both = [jnp.where(left, here, 0.0), jnp.where(left, 0.0, here)]
    return jnp.concatenate(both, axis=0).astype(BF16)


def pack_kernel(wk_ref, wv_ref, w_ref):
    units = wk_ref.shape[0]
    w_ref[0:units] = wk_ref[...]
    w_ref[units:] = wv_ref[...]


def pair_kernel(pair_ref, out_ref):
    a, b = pair_ref[0].astype(F32), pair_ref[1].astype(F32)
    last = b[64:65] + b[65:66]
    state = (a[0:64] * jnp.exp(last) + b[0:64]).astype(BF16)
    recall = jnp.broadcast_to(b[68:69], (8, b.shape[1])).astype(BF16)
    own = [
        dot(recall[:, at], apart(a[0:64], at), NT)[0:1]
        for at in (slice(128 * p, 128 * p + 128) for p in range(b.shape[1] // 128))
    ]
    own = b[66:67] + b[67:68] + jnp.concatenate(own, axis=1)
    start = a[64:65] + a[65:66]
    tail = lines(*hi_lo(start + last), *hi_lo(own), b[68:69] * jnp.exp(start), b[69:70], b[70:71])
    for n in range(out_ref.shape[0]):
        out_ref[n, 0:64] = state
        out_ref[n, 64:72] = tail


def middle_kernel(
    chip_ref, core_ref, all_ref, pair_ref, own_ref, rec_ref, skip_ref, gate_ref, gn_ref, ln_ref,
    mid_ref, main_ref, side_ref,
):
    rows, width = own_ref.shape
    main = main_ref.shape[0]

    def join(ref):
        def step(i, state):
            piece = ref[i].astype(F32)
            return state * jnp.exp(piece[64:65] + piece[65:66]) + piece[0:64]

        return step

    chip, core = chip_ref[0], core_ref[0]
    split = jnp.maximum(chip + core - 1, 0)
    old = lax.fori_loop(0, split, join(all_ref), jnp.zeros((64, width), F32))
    state = lax.fori_loop(split, chip, join(all_ref), old)
    state = lax.fori_loop(0, core, join(pair_ref), state)

    def finish(own, recall, skip, gate, before, at):
        left = iota(own.shape, 1) < 64

        def mean(x):
            a = jnp.sum(jnp.where(left, x, 0.0), axis=1, keepdims=True)
            b = jnp.sum(jnp.where(left, 0.0, x), axis=1, keepdims=True)
            return jnp.where(left, a, b) * (1.0 / 64)

        wkv = own + dot(recall, apart(before, at), NT)
        centre = wkv - mean(wkv)
        normed = centre * lax.rsqrt(mean(centre * centre) + EPS_GROUP)
        normed = normed * gn_ref[0:1, at] + gn_ref[1:2, at]
        return skip + normed * (gate / (1.0 + jnp.exp(-gate)))

    line = iota((8, 128), 0)
    prior = all_ref[jnp.maximum(chip - 1, 0)].astype(F32)[64:72]
    prior = jnp.where(core > 0, pair_ref[0].astype(F32)[64:72], prior)
    prior = [prior[2:3] + prior[3:4], prior[4:5], prior[5:6], prior[6:7]]
    for p in range(width // 128):
        at = slice(128 * p, 128 * p + 128)
        middle = finish(
            own_ref[:, at], rec_ref[:, at], skip_ref[:, at].astype(F32), gate_ref[:, at].astype(F32), state, at
        )
        mid_ref[:, at] = middle
        main_ref[:, at] = middle[0:main].astype(BF16)
        own, recall, skip, gate = (jnp.broadcast_to(row[:, at], (8, 128)) for row in prior)
        tail = jnp.where(line == 0, finish(own, recall.astype(BF16), skip, gate, old, at), 0.0)
        for n in range(3):
            hi, lo = hi_lo(ln_ref[n : n + 1, at])
            tail = jnp.where(line == 2 * n + 1, hi.astype(F32), tail)
            tail = jnp.where(line == 2 * n + 2, lo.astype(F32), tail)
        edge, tail = middle[main:].astype(BF16), tail.astype(BF16)
        for g in range(side_ref.shape[0]):
            side_ref[g, 0, :, at] = edge
            side_ref[g, 1, :, at] = tail


def ffn_kernel(seq_ref, zh_ref, main_ref, side_ref, w_hbm, give_ref, hidden_ref, w_ref, sems):
    _, rows, width = give_ref.shape
    groups, main = main_ref.shape[0:2]
    full = groups * width
    depth = w_hbm.shape[1]
    tall = w_hbm.shape[0] // (full // depth)
    units = tall // 2
    chunks = sems.shape[0]
    step = full // chunks

    def copy(q):
        at = pl.ds(q * step // depth * tall, step // depth * tall)
        return pltpu.make_async_copy(w_hbm.at[at], w_ref.at[at], sems.at[q])

    def weights(g, first):
        starts = [(g * (width // depth) + b) * tall + first for b in range(width // depth)]
        if not isinstance(g, int):
            starts = [pl.multiple_of(start, 64) for start in starts]
        return jnp.concatenate([w_ref[pl.ds(start, units)] for start in starts], axis=1)

    for q in range(chunks):
        copy(q).start()

    def load(g):
        return jnp.concatenate([main_ref[g].astype(F32), side_ref[g, 0].astype(F32)], axis=0)

    def stats(get, n):
        first, second = jnp.zeros((n, width), F32), jnp.zeros((n, width), F32)
        for g in range(groups):
            x = get(g)
            first, second = first + x, second + x * x
        mu = jnp.sum(first, axis=1, keepdims=True) / full
        var = jnp.sum(second, axis=1, keepdims=True) / full - mu * mu
        return mu, lax.rsqrt(var + EPS_LAYER)

    mu, scale = stats(load, rows)
    pmu, pscale = stats(lambda g: side_ref[g, 1].astype(F32)[0:1], 1)
    live = seq_ref[0] > 0
    head = iota((rows, width), 0) == 0
    acc = jnp.zeros((rows, units), F32)
    for g in range(groups):
        side = side_ref[g, 1].astype(F32)
        gain, bias, blend = (side[n : n + 1] + side[n + 1 : n + 2] for n in (1, 3, 5))
        xn = ((load(g) - mu) * scale * gain + bias).astype(BF16).astype(F32)
        pn = ((side[0:1] - pmu) * pscale * gain + bias).astype(BF16).astype(F32)
        pn = jnp.where(live, pn, 0.0)
        prev = jnp.where(head, pn, pltpu.roll(xn, 1, 0))
        xk = (xn + (prev - xn) * blend).astype(BF16)
        if g * width % step == 0:
            copy(g * width // step).wait()
        acc = acc + dot(xk, weights(g, 0), NT)
    hidden = jnp.square(jnp.maximum(acc, 0.0)).astype(BF16)
    hidden_ref[...] = hidden
    for g in range(groups // 2):
        give_ref[g] = dot(hidden, weights(2 * g + 1 - zh_ref[0], units), NN).astype(BF16)


def keep_kernel(zh_ref, hidden_ref, w_hbm, keep_ref, w_ref, sems):
    groups, rows, width = keep_ref.shape
    units = hidden_ref.shape[1]
    depth = w_hbm.shape[1]
    each = width // depth

    def copy(g, b):
        start = (((2 * g + zh_ref[0]) * each + b) * 2 + 1) * units
        return pltpu.make_async_copy(
            w_hbm.at[pl.ds(pl.multiple_of(start, 64), units)], w_ref.at[g * each + b], sems.at[g * each + b]
        )

    for g in range(groups):
        for b in range(each):
            copy(g, b).start()
    for g in range(groups):
        for b in range(each):
            copy(g, b).wait()
        w = jnp.concatenate([w_ref[g * each + b] for b in range(each)], axis=1)
        keep_ref[g] = dot(hidden_ref[...], w, NN).astype(BF16)


VMEM = functools.partial(pl.BlockSpec, memory_space=pltpu.VMEM)
SMEM = functools.partial(pl.BlockSpec, memory_space=pltpu.SMEM)


def near(x):
    return pltpu.with_memory_space_constraint(x, pltpu.VMEM)


def make(interpret):
    def call(kernel, outs, *args, in_specs=None, **more):
        return pl.pallas_call(
            kernel,
            out_shape=[pltpu.HBM(s, t) if len(s) == 2 and s[0] > 512 else pltpu.VMEM(s, t) for s, t in outs],
            in_specs=in_specs or [VMEM() for _ in args],
            out_specs=[VMEM() for _ in outs],
            interpret=interpret,
            **more,
        )(*args)

    def local(
        skip, recept, keys, values, gating, logit, boost, gn_gain, gn_bias, ln_gain, ln_bias, blend, wk, wv
    ):
        rows, width = skip.shape
        groups = lax.axis_size(HID)
        blocks = lax.axis_size(SEQ)
        at_seq = lax.axis_index(SEQ).reshape(1)

        chips = blocks // lax.axis_size("c")
        chip = lax.axis_index(("y", "x")).reshape(1)
        core = lax.axis_index("c").reshape(1)
        zh = lax.axis_index("zh").reshape(1)
        (weights,) = call(pack_kernel, [((2 * wk.shape[1], wk.shape[0]), BF16)], wk.T, wv.T)
        own, recall, state = call(
            wkv_kernel,
            [((rows, width), F32), ((rows, width), BF16), ((72, width), BF16)],
            recept, keys, values, logit, boost, skip, gating,
        )
        weights = lax.all_gather(weights, SEQ, tiled=True)
        pair = lax.all_gather(state, "c")
        (states,) = call(pair_kernel, [((chips, 72, width), BF16)], near(pair))
        states = lax.all_to_all(states, ("y", "x"), 0, 0, tiled=True)
        middle, main, side = call(
            middle_kernel,
            [((rows, width), F32), ((rows - 8, width), BF16), ((groups, 2, 8, width), BF16)],
            chip, core, near(states), near(pair), near(own), near(recall), skip, gating,
            jnp.stack([gn_gain, gn_bias]), jnp.stack([ln_gain, ln_bias, blend]),
            in_specs=[SMEM(), SMEM()] + [VMEM()] * 8,
        )
        side = lax.all_to_all(side, HID, 0, 0, tiled=True)
        main = lax.all_gather(main, HID)
        any_space = pl.BlockSpec(memory_space=pl.ANY)
        units, depth = wk.shape[1], wk.shape[0]
        give, hidden = call(
            ffn_kernel,
            [((groups // 2, rows, width), BF16), ((rows, units), BF16)],
            at_seq, zh, near(main), near(side), weights,
            in_specs=[SMEM(), SMEM(), VMEM(), VMEM(), any_space],
            scratch_shapes=[pltpu.VMEM(weights.shape, BF16), pltpu.SemaphoreType.DMA((min(8, groups),))],
        )
        give = lax.ppermute(give, "zh", [(0, 1), (1, 0)])
        (keep,) = call(
            keep_kernel,
            [((groups // 2, rows, width), BF16)],
            zh, near(hidden), weights,
            in_specs=[SMEM(), VMEM(), any_space],
            scratch_shapes=[pltpu.VMEM((blocks // 2, units, depth), BF16), pltpu.SemaphoreType.DMA((blocks // 2,))],
        )
        part = (keep.astype(F32) + give.astype(F32)).astype(BF16)
        part = lax.all_to_all(part, "zl", 0, 0, tiled=True)
        return (middle + jnp.sum(part.astype(F32), axis=0)).astype(BF16)

    return local


def build(finer, interpret=False):
    tile, vec = P(SEQ, HID), P(HID)
    return jax.shard_map(
        make(interpret),
        mesh=finer,
        in_specs=(tile,) * 6 + (P(HID, None),) + (vec,) * 5 + (tile, tile),
        out_specs=tile,
        check_vma=False,
    )


def solution(mesh):
    return build(Mesh(mesh.devices.reshape(4, 4, 2, mesh.shape["hid"] // 2, 2), (*SEQ, *HID)))
```
